256 devices in a mesh: coil: 4 (over z_lo), spoke: 64 (over y, z_hi, x, core).
Axes of the slice: x: 4, y: 4, z: 8 (z_hi: 2, z_lo: 4; z = z_hi * 4 + z_lo), core: 2. Of those that a mesh axis runs over, the one named last changes fastest.
Arguments:
- image: float32 [256, 2, 2, 256], P('spoke'), may hold values from -6 to 6
- residual: float32 [256, 2, 2, 256], P('spoke'), may hold values from -12 to 12
- direction: float32 [256, 2, 2, 256], P('spoke'), may hold values from -12 to 12
- coil_maps: bfloat16 [256, 32, 2, 2, 256], P(None, 'coil'), may hold values from -0.75 to 0.75
- interp_weights: bfloat16 [512, 128, 2048], P('spoke'), may hold values from -0.125 to 0.125
- tile_index: int32 [512], P('spoke'), may hold values from 0 to 31
Outputs:
- new_image: float32 [256, 2, 2, 256], P('spoke')
- new_residual: float32 [256, 2, 2, 256], P('spoke')
- new_direction: float32 [256, 2, 2, 256], P('spoke')
The draws below stay inside these ranges and needn't reach their ends.
All inputs are finite; a program needn't handle non-finite values.
Results may differ from the reference program's by a relative error of at most 0.0017.
Values may be sent and summed in bfloat16 or wider, within the bound.
A program may use at most 128 MiB of HBM per device.

```python
import math
import jax
import jax.numpy as jnp
from jax import lax

NY = 256
NX = 256
COILS = 32
PLANES = 2
TR = 8
SB = 128
NBLK = 8
BLOCKS = 512
TC = 2048
N_COIL = 4
N_SPOKE = 64


def rising_field(key):
    height = jnp.arange(NY, dtype=jnp.float32)[:, None, None, None] / (NY - 1)
    values = jnp.clip(jax.random.normal(key, (NY, PLANES, 2, NX), jnp.float32), -4.0, 4.0)
    return values * (1.0 + 2.0 * height)


def draw_residual(key, part):
    return rising_field(jax.random.fold_in(key, 17))


def draw_direction(key, part):
    return rising_field(jax.random.fold_in(key, 29))


def place_ends(drawn, stream_key, low, largest):
    shape = drawn.shape
    spot = [jax.random.randint(jax.random.fold_in(stream_key, axis), (), 0, shape[axis]) for axis in range(len(shape))]
    drawn = drawn.at[tuple(spot)].set(low)
    longest = shape.index(max(shape))
    spot[longest] = (spot[longest] + 1) % shape[longest]
    return drawn.at[tuple(spot)].set(largest)


def level_of(rng, extent, shards, low, high):
    factor_of, own = 1.0, jax.random.fold_in(rng, 6)
    for dim, parts in shards:
        steps = jnp.exp(jax.random.uniform(jax.random.fold_in(own, dim), (parts,), jnp.float32, low / len(shards), high / len(shards)))
        factor_of = factor_of * jnp.repeat(steps, extent[dim] // parts).reshape([-1 if axis == dim else 1 for axis in range(len(extent))])
    return factor_of


def normal_values(rng, dims, scale, limit, shards=(), kind=jnp.bfloat16):
    drawn = jax.random.normal(rng, dims, jnp.float32) * scale
    if len(shards) > 0:
        drawn = level_of(rng, dims, shards, -0.22, 0.18) * drawn
    return jnp.clip(drawn, min=-limit, max=limit).astype(kind)


def setup_inputs(seed: int = 0) -> dict:
    splits = jax.random.split(jax.random.key(seed), 7)
    image = normal_values(splits[0], (NY, PLANES, 2, NX), 1.0, 6.0, ((0, 64),), jnp.float32)
    residual = draw_residual(jax.random.fold_in(splits[6], 71), 0)
    direction = draw_direction(jax.random.fold_in(splits[6], 71), 0)
    coil_maps = normal_values(splits[3], (NY, COILS, PLANES, 2, NX), (2 * COILS) ** -0.5, 0.75, ((1, 4),))
    interp_weights = normal_values(splits[4], (BLOCKS, SB, TC), TC ** -0.5, 0.125, ((0, 64),))
    tile_index = place_ends(jax.random.randint(splits[5], (BLOCKS,), 0, NY // TR), jax.random.fold_in(splits[5], 1), 0, (NY // TR) - 1).astype(jnp.int32)
    return dict(image=image, residual=residual, direction=direction, coil_maps=coil_maps, interp_weights=interp_weights, tile_index=tile_index)


ridge = 0.1

def wave_tables(first, second, length):
    phase = first[:, None] * second[None, :] % length
    angle = phase.astype(jnp.float32) * (2.0 * math.pi / length)
    factor = 1.0 / math.sqrt(length)
    return ((jnp.cos(angle) * factor).astype(jnp.bfloat16), (jnp.sin(angle) * factor).astype(jnp.bfloat16))

def row_tables():
    lines = jnp.arange(NX, dtype=jnp.int32)
    cosines, sines = wave_tables(lines, lines, NX)
    forward_row = jnp.concatenate([jnp.concatenate([cosines, -sines], 1), jnp.concatenate([sines, cosines], 1)], 0)
    inverse_row = jnp.concatenate([jnp.concatenate([cosines, sines], 1), jnp.concatenate([-sines, cosines], 1)], 0)
    return (forward_row, inverse_row)

def coil_spectra(maps_rows, field_rows, forward_row):
    maps_real = maps_rows[..., 0, :].astype(jnp.float32)
    maps_imag = maps_rows[..., 1, :].astype(jnp.float32)
    field_real = field_rows[:, None, :, 0, :]
    field_imag = field_rows[:, None, :, 1, :]
    coil_real = maps_real * field_real - maps_imag * field_imag
    coil_imag = maps_real * field_imag + maps_imag * field_real
    coil_image = jnp.stack([coil_real, coil_imag], -2).astype(jnp.bfloat16)
    spectra = jnp.dot(coil_image.reshape(-1, 2 * NX), forward_row, preferred_element_type=jnp.float32)
    return spectra.astype(jnp.bfloat16).reshape(coil_image.shape)

def combine_coils(maps_rows, images):
    maps_real = maps_rows[..., 0, :].astype(jnp.float32)
    maps_imag = maps_rows[..., 1, :].astype(jnp.float32)
    image_real = images[..., 0, :]
    image_imag = images[..., 1, :]
    combined_real = lax.optimization_barrier(jnp.sum(maps_real * image_real + maps_imag * image_imag, axis=1))
    combined_imag = lax.optimization_barrier(jnp.sum(maps_real * image_imag - maps_imag * image_real, axis=1))
    return jnp.stack([combined_real, combined_imag], -2)

def reference(image, residual, direction, coil_maps, interp_weights, tile_index):
    forward_row, inverse_row = row_tables()
    lines = jnp.arange(NY, dtype=jnp.int32)
    cosines, sines = wave_tables(lines, lines, NY)
    group_coils = COILS // N_COIL
    flat_width = group_coils * PLANES * 2 * NX
    block_index = tile_index.reshape(N_SPOKE, NBLK).astype(jnp.int32)
    block_weights = interp_weights.reshape(N_SPOKE, NBLK, SB, TR, NX)
    combined = jnp.zeros((NY, PLANES, 2, NX), jnp.float32)
    for group in range(N_COIL):
        maps_group = coil_maps[:, group * group_coils:(group + 1) * group_coils]
        spectra = coil_spectra(maps_group, direction, forward_row).reshape(NY, flat_width)
        first = jnp.dot(cosines, spectra, preferred_element_type=jnp.float32).reshape(NY, group_coils, PLANES, 2, NX)
        second = jnp.dot(sines, spectra, preferred_element_type=jnp.float32).reshape(NY, group_coils, PLANES, 2, NX)
        kspace = jnp.stack([first[..., 0, :] + second[..., 1, :], first[..., 1, :] - second[..., 0, :]], -2)
        kspace = kspace.astype(jnp.bfloat16).reshape(NY // TR, TR, group_coils, PLANES, 2, NX)

        def grid_device(total, inputs):
            indices, weights = inputs
            picked = kspace[indices].astype(jnp.float32)
            weights_wide = weights.astype(jnp.float32)
            samples = jnp.einsum('btcpax,bjtx->bcpaj', picked, weights_wide, precision=lax.Precision.HIGHEST)
            samples = samples.astype(jnp.bfloat16).astype(jnp.float32)
            gridded = jnp.einsum('bcpaj,bjtx->btcpax', samples, weights_wide, precision=lax.Precision.HIGHEST)
            gridded = gridded.astype(jnp.bfloat16)
            spread = jnp.dot(gridded.reshape(-1, 2 * NX), inverse_row, preferred_element_type=jnp.float32)
            spread = spread.astype(jnp.bfloat16).astype(jnp.float32).reshape(NBLK, TR, group_coils, PLANES, 2, NX)
            return (total.at[indices].add(spread), None)
        start_total = jnp.zeros((NY // TR, TR, group_coils, PLANES, 2, NX), jnp.float32)
        gridded_total, unused = lax.scan(grid_device, start_total, (block_index, block_weights))
        gridded_total = gridded_total.reshape(NY, flat_width)
        first = jnp.dot(cosines.astype(jnp.float32), gridded_total, precision=lax.Precision.HIGHEST)
        second = jnp.dot(sines.astype(jnp.float32), gridded_total, precision=lax.Precision.HIGHEST)
        first = first.reshape(NY, group_coils, PLANES, 2, NX)
        second = second.reshape(NY, group_coils, PLANES, 2, NX)
        images = jnp.stack([first[..., 0, :] - second[..., 1, :], first[..., 1, :] + second[..., 0, :]], -2)
        combined = combined + combine_coils(maps_group, images)
    applied = combined + ridge * direction
    norm_now = jnp.sum(residual * residual)
    alpha = norm_now / jnp.sum(direction * applied)
    new_image = image + alpha * direction
    new_residual = residual - alpha * applied
    norm_next = jnp.sum(new_residual * new_residual)
    new_direction = new_residual + norm_next / norm_now * direction
    return (new_image, new_residual, new_direction)
```

```python
import math

import jax
import jax.numpy as jnp
import numpy as np
from jax import lax
from jax.experimental import pallas as pl
from jax.experimental.pallas import tpu as pltpu
from jax.sharding import PartitionSpec as P

F32, BF16 = jnp.float32, jnp.bfloat16
MESH = pl.DeviceIdType.MESH
ridge = 0.1


class Place:
    def __init__(self):
        self.coil = lax.axis_index("coil")
        self.spoke = lax.axis_index("spoke")
        self.core = self.spoke % 2
        self.x = (self.spoke // 2) % 4
        self.hi = (self.spoke // 8) % 2
        self.y = self.spoke // 16
        self.z = self.hi * 4 + self.coil
        self.sibling = self.spoke + 1 - 2 * self.core
        self.other = self.spoke + 8 - 16 * self.hi

    def chip(self, j):
        q = (self.y * 4 + self.x + j) % 16
        return (q // 4) * 16 + self.hi * 8 + (q % 4) * 2 + self.core

    def in_plane(self, j):
        return (self.y * 8 + self.x * 2 + self.core + j) % 32


def spoke_of(q, hi):
    return (q // 8) * 16 + hi * 8 + q % 8


def signal(device):
    pl.semaphore_signal(pltpu.get_barrier_semaphore(), inc=1, device_id=device, device_id_type=MESH)


def remote(src, dst, send_sem, recv_sem, device):
    return pltpu.make_async_remote_copy(
        src_ref=src, dst_ref=dst, send_sem=send_sem, recv_sem=recv_sem,
        device_id=device, device_id_type=MESH,
    )


def gather_kernel(d_ref, out_ref, own, send_sem, recv_sem):
    here = Place()
    coil, spoke, sibling, other = here.coil, here.spoke, here.sibling, here.other
    for k in range(8):
        own[2 * k:2 * k + 2, :] = d_ref[k // 2, k % 2]

    def greet(j, carry):
        signal((coil, here.chip(j)))
        return carry

    lax.fori_loop(1, 16, greet, 0)
    signal((coil, sibling))
    signal((3 - coil, other))
    out_ref[spoke] = own[...]
    pl.semaphore_wait(pltpu.get_barrier_semaphore(), 17)

    def send(src, slot, phase, j, device):
        return remote(src, out_ref.at[slot], send_sem.at[phase, j], recv_sem.at[slot], device)

    def arrived(slot):
        remote(own, out_ref.at[slot], send_sem.at[0, 0], recv_sem.at[slot], (coil, sibling)).wait_recv()

    send(own, spoke, 2, 0, (3 - coil, other)).start()

    def first(j, carry):
        send(own, spoke, 0, j, (coil, here.chip(j))).start()
        return carry

    lax.fori_loop(1, 16, first, 0)
    send(own, spoke, 0, 0, (coil, sibling)).start()
    arrived(other)

    def second(j, carry):
        send(out_ref.at[other], other, 1, j, (coil, here.chip(j))).start()
        return carry

    lax.fori_loop(1, 16, second, 0)
    send(out_ref.at[other], other, 1, 0, (coil, sibling)).start()
    flip = 8 - 16 * here.hi
    for phase, shift in ((2, 0), (3, flip)):
        def forward(j, carry, phase=phase, shift=shift):
            slot = here.chip(j) + shift
            arrived(slot)
            send(out_ref.at[slot], slot, phase, j, (coil, sibling)).start()
            return carry

        lax.fori_loop(1, 16, forward, 0)

    def rest(j, carry):
        slot = here.chip(j) + 1 - 2 * here.core
        arrived(slot)
        arrived(slot + flip)
        return carry

    lax.fori_loop(0, 16, rest, 0)
    for phase in range(4):
        def sent(j, carry, phase=phase):
            send(own, spoke, phase, j, (coil, sibling)).wait_send()
            return carry

        lax.fori_loop(1 if phase == 3 else 0, 16, sent, 0)


def gather_call(direction):
    vm = pl.BlockSpec(memory_space=pltpu.VMEM)
    return pl.pallas_call(
        gather_kernel,
        out_shape=jax.ShapeDtypeStruct((64, 16, 256), F32),
        in_specs=[vm],
        out_specs=vm,
        scratch_shapes=[
            pltpu.VMEM((16, 256), F32),
            pltpu.SemaphoreType.DMA((4, 16)),
            pltpu.SemaphoreType.DMA((64,)),
        ],
        compiler_params=pltpu.CompilerParams(collective_id=0, has_side_effects=True),
        name="gather",
    )(direction)


def reduce_kernel(part_ref, d_ref, r_ref, applied_ref, total_ref,
                  came, zsend, zcame, d16, r16, row, rows, send_sem, recv_sem, zsend_sem, zrecv_sem,
                  ssend_sem, srecv_sem):
    here = Place()
    coil, spoke, hi, z = here.coil, here.spoke, here.hi, here.z
    me = here.in_plane(0)

    def greet(j, carry):
        signal((coil, spoke_of(here.in_plane(j), hi)))
        return carry

    def greet_across(j, carry):
        signal((3 - coil, spoke_of(j, 1 - hi)))
        return carry

    def line(j):
        to = (z + j) % 8
        return to, (to % 4, spoke + 8 * (to // 4 - hi))

    def greet_line(j, carry):
        to, device = line(j)

        @pl.when(to != 7 - z)
        def _():
            signal(device)

        return carry

    lax.fori_loop(1, 32, greet, 0)
    lax.fori_loop(0, 32, greet_across, 0)
    lax.fori_loop(1, 8, greet_line, 0)
    for k in range(8):
        d16[2 * k:2 * k + 2, :] = d_ref[k // 2, k % 2]
        r16[2 * k:2 * k + 2, :] = r_ref[k // 2, k % 2]
    pl.semaphore_wait(pltpu.get_barrier_semaphore(), 69)

    def exchange(j):
        q = here.in_plane(j)
        return remote(part_ref.at[q // 8, :, q % 8], came.at[me], send_sem.at[j], recv_sem.at[me],
                      (coil, spoke_of(q, hi)))

    def start(j, carry):
        exchange(j).start()
        return carry

    lax.fori_loop(1, 32, start, 0)
    came[me] = part_ref[here.y, :, here.x * 2 + here.core]

    def came_in(j, carry):
        q = here.in_plane(j)
        remote(came.at[q], came.at[q], send_sem.at[j], recv_sem.at[q], (coil, spoke)).wait_recv()
        return carry

    lax.fori_loop(1, 32, came_in, 0)
    total = came[0].astype(F32)
    for q in range(1, 32):
        total = total + came[q].astype(F32)
    zsend[...] = total.astype(BF16)

    def zcopy(j):
        to, device = line(j)
        return remote(zsend.at[to // 4], zcame.at[z], zsend_sem.at[j], zrecv_sem.at[z], device)

    def zstart(j, carry):
        zcopy(j).start()
        return carry

    lax.fori_loop(1, 8, zstart, 0)
    zcame[z] = zsend[hi]

    def zwait(j, carry):
        frm = (z + j) % 8
        remote(zsend.at[0], zcame.at[frm], zsend_sem.at[j], zrecv_sem.at[frm], (coil, spoke)).wait_recv()
        return carry

    lax.fori_loop(1, 8, zwait, 0)
    applied = zcame[0].astype(F32)
    for k in range(1, 8):
        applied = applied + zcame[k].astype(F32)
    d, r = d16[...], r16[...]
    applied = applied + ridge * d
    sums = [jnp.sum(r * r), jnp.sum(d * applied), jnp.sum(r * applied), jnp.sum(applied * applied)]
    lane = lax.broadcasted_iota(jnp.int32, (1, 128), 1)
    line_of = jnp.zeros((1, 128), F32)
    for k, value in enumerate(sums):
        line_of = jnp.where(lane == k, value, line_of)
    row[...] = line_of
    rows[spoke] = line_of

    def share(j):
        return remote(row, rows.at[spoke], ssend_sem.at[j], srecv_sem.at[spoke],
                      (coil, spoke_of(here.in_plane(j), hi)))

    def share_across(j):
        return remote(row, rows.at[spoke], ssend_sem.at[32 + j], srecv_sem.at[spoke],
                      (3 - coil, spoke_of(here.in_plane(j), 1 - hi)))

    def share_start(j, carry):
        share(j).start()
        return carry

    def across_start(j, carry):
        share_across(j).start()
        return carry

    lax.fori_loop(0, 32, across_start, 0)
    lax.fori_loop(1, 32, share_start, 0)
    for k in range(8):
        applied_ref[k // 2, k % 2] = applied[2 * k:2 * k + 2]

    def share_wait(j, carry):
        frm = (spoke + j) % 64
        remote(row, rows.at[frm], ssend_sem.at[j], srecv_sem.at[frm], (coil, spoke)).wait_recv()
        return carry

    lax.fori_loop(1, 64, share_wait, 0)
    total_ref[...] = jnp.sum(rows[...], axis=0)

    def sent(j, carry):
        exchange(j).wait_send()
        share(j).wait_send()
        return carry

    def zsent(j, carry):
        zcopy(j).wait_send()
        return carry

    def across_sent(j, carry):
        share_across(j).wait_send()
        return carry

    lax.fori_loop(1, 32, sent, 0)
    lax.fori_loop(1, 8, zsent, 0)
    lax.fori_loop(0, 32, across_sent, 0)


def reduce_call(parts, direction, residual):
    vm = pl.BlockSpec(memory_space=pltpu.VMEM)
    return pl.pallas_call(
        reduce_kernel,
        out_shape=(jax.ShapeDtypeStruct((4, 2, 2, 256), F32), jax.ShapeDtypeStruct((1, 128), F32)),
        in_specs=[vm] * 3,
        out_specs=(vm, vm),
        scratch_shapes=[
            pltpu.VMEM((32, 2, 16, 256), BF16),
            pltpu.VMEM((2, 16, 256), BF16),
            pltpu.VMEM((8, 16, 256), BF16),
            pltpu.VMEM((16, 256), F32),
            pltpu.VMEM((16, 256), F32),
            pltpu.VMEM((1, 128), F32),
            pltpu.VMEM((64, 1, 128), F32),
            pltpu.SemaphoreType.DMA((32,)),
            pltpu.SemaphoreType.DMA((32,)),
            pltpu.SemaphoreType.DMA((8,)),
            pltpu.SemaphoreType.DMA((8,)),
            pltpu.SemaphoreType.DMA((64,)),
            pltpu.SemaphoreType.DMA((64,)),
        ],
        compiler_params=pltpu.CompilerParams(collective_id=1, has_side_effects=True),
        name="reduce",
    )(parts.reshape(4, 2, 8, 16, 256), direction, residual)


def wave_block():
    n = 256
    q = (np.arange(n)[:, None] * np.arange(n)[None, :]) % n
    ang = q.astype(np.float32) * np.float32(2.0 * math.pi / n)
    c = (np.cos(ang) * np.float32(1.0 / math.sqrt(n))).astype(jnp.bfloat16)
    s = (np.sin(ang) * np.float32(1.0 / math.sqrt(n))).astype(jnp.bfloat16)
    return np.concatenate([np.concatenate([c, s], 1), np.concatenate([-s, c], 1)], 0)

def dot(a, b, dims=(((1,), (0,)), ((), ()))):
    return lax.dot_general(a, b, dims, preferred_element_type=F32)

def grid_kernel(tile_ref, dirg_ref, maps_ref, wave_ref, w_hbm, out_ref,
                dirf, d, tf, tft, tr, ti, ks, gr, gi, acc, wv, sem):
    wcopy = pltpu.make_async_copy(w_hbm, wv, sem)
    wcopy.start()
    for b in range(8):
        t = tile_ref[b]
        tf[pl.ds(b * 8, 8), :] = wave_ref[pl.ds(pl.multiple_of(t * 8, 8), 8), :]
        tf[pl.ds(64 + b * 8, 8), :] = wave_ref[pl.ds(pl.multiple_of(256 + t * 8, 8), 8), :]
    tft[...] = tf[...].astype(F32).T.astype(BF16)
    for h in range(2):
        dirf[h] = dirg_ref[:, :, h * 128:(h + 1) * 128].reshape(1024, 128).astype(F32)
        for q in range(4):
            for r in range(4):
                d[q, h, pl.ds(r, 64, stride=4), :] = dirf[h, pl.ds(r * 4 + q, 64, stride=16), :]
    acc[...] = jnp.zeros_like(acc)

    def forward(i, carry):
        p, c = i // 8, i % 8
        mr = maps_ref[p, c, 0].astype(F32)
        mi = maps_ref[p, c, 1].astype(F32)
        dr = jnp.concatenate([d[2 * p, 0], d[2 * p, 1]], 1)
        di = jnp.concatenate([d[2 * p + 1, 0], d[2 * p + 1, 1]], 1)
        cr = (mr * dr - mi * di).astype(BF16)
        ci = (mr * di + mi * dr).astype(BF16)
        t = dot(tf[:, :256], cr) + dot(tf[:, 256:], ci)
        rows = pl.ds(pl.multiple_of(i * 64, 64), 64)
        tr[rows, :] = t[:64].astype(BF16)
        ti[rows, :] = t[64:].astype(BF16)
        return carry
    lax.fori_loop(0, 16, forward, 0, unroll=2)

    cosm, sinm, nsinm = wave_ref[:256, :256], wave_ref[:256, 256:], wave_ref[256:, :256]

    def halves(rows, re, im):
        for h in range(2):
            ks[0, h, rows, :] = re[:, h * 128:(h + 1) * 128]
            ks[1, h, rows, :] = im[:, h * 128:(h + 1) * 128]

    def strided(part, rows):
        return jnp.concatenate([ks[part, 0, rows, :], ks[part, 1, rows, :]], 1)

    def row(i, carry):
        rows = pl.ds(pl.multiple_of(i * 256, 256), 256)
        a, b = tr[rows, :], ti[rows, :]
        halves(rows, dot(a, cosm) + dot(b, sinm), dot(a, nsinm) + dot(b, cosm))
        return carry
    lax.fori_loop(0, 4, row, 0)
    wcopy.wait()

    def block(b, carry):
        parts = []
        for r in range(8):
            rows = pl.ds(b * 8 + r, 16, stride=64)
            re, im = strided(0, rows), strided(1, rows)
            parts.append(jnp.concatenate([re, im], 0).astype(BF16))
        picked = jnp.concatenate(parts, 1)
        w = wv[b]
        s = dot(picked, w, (((1,), (1,)), ((), ()))).astype(BF16)
        g = dot(s, w).astype(BF16)
        for r in range(8):
            rows = pl.ds(pl.multiple_of((b * 8 + r) * 16, 16), 16)
            gr[rows, :] = g[:16, r * 256:(r + 1) * 256]
            gi[rows, :] = g[16:, r * 256:(r + 1) * 256]
        return carry
    lax.fori_loop(0, 8, block, 0, unroll=2)

    def back(i, carry):
        rows = pl.ds(pl.multiple_of(i * 256, 256), 256)
        a, b = gr[rows, :], gi[rows, :]
        halves(rows, dot(a, cosm) + dot(b, nsinm), dot(a, sinm) + dot(b, cosm))
        return carry
    lax.fori_loop(0, 4, back, 0)

    def combine(i, carry):
        p, c = i // 8, i % 8
        rows = pl.ds(i, 64, stride=16)
        sr, si = strided(0, rows), strided(1, rows)
        sp = jnp.concatenate([sr, si], 0).astype(BF16)
        img = dot(tft[...], sp)
        mr = maps_ref[p, c, 0].astype(F32)
        mi = maps_ref[p, c, 1].astype(F32)
        re = mr * img[:256] + mi * img[256:]
        im = mr * img[256:] - mi * img[:256]
        for h in range(2):
            acc[2 * p, h] += re[:, h * 128:(h + 1) * 128]
            acc[2 * p + 1, h] += im[:, h * 128:(h + 1) * 128]
        return carry
    lax.fori_loop(0, 16, combine, 0, unroll=2)
    for h in range(2):
        for q in range(4):
            for r in range(4):
                dirf[h, pl.ds(r * 4 + q, 64, stride=16), :] = acc[q, h, pl.ds(r, 64, stride=4), :]
        out_ref[:, :, h * 128:(h + 1) * 128] = dirf[h].astype(BF16).reshape(64, 16, 128)

def grid_call(tile_index, dirg, maps_t, wave, w):
    vm = pl.BlockSpec(memory_space=pltpu.VMEM)
    return pl.pallas_call(
        grid_kernel,
        out_shape=jax.ShapeDtypeStruct((64, 16, 256), BF16),
        in_specs=[pl.BlockSpec(memory_space=pltpu.SMEM), vm, vm, vm, pl.BlockSpec(memory_space=pl.ANY)],
        out_specs=vm,
        scratch_shapes=[
            pltpu.VMEM((2, 1024, 128), F32), pltpu.VMEM((4, 2, 256, 128), F32),
            pltpu.VMEM((128, 512), BF16), pltpu.VMEM((512, 128), BF16),
            pltpu.VMEM((1024, 256), BF16), pltpu.VMEM((1024, 256), BF16),
            pltpu.VMEM((2, 2, 1024, 128), F32),
            pltpu.VMEM((1024, 256), BF16), pltpu.VMEM((1024, 256), BF16),
            pltpu.VMEM((4, 2, 256, 128), F32),
            pltpu.VMEM((8, 128, 2048), BF16), pltpu.SemaphoreType.DMA],
        compiler_params=pltpu.CompilerParams(vmem_limit_bytes=60 * 2**20),
        name="grid",
    )(tile_index, dirg, maps_t, wave, w)


def shards(image, residual, direction, coil_maps, interp_weights, tile_index):
    maps = jnp.transpose(coil_maps, (2, 1, 3, 0, 4))
    whole = gather_call(direction)
    parts = grid_call(tile_index, whole, maps, jnp.asarray(wave_block()), interp_weights)
    applied, total = reduce_call(parts, direction, residual)
    norm_now, curvature, crossing, squared = (total[0, k] for k in range(4))
    alpha = norm_now / curvature
    new_residual = residual - alpha * applied
    norm_next = norm_now - 2.0 * alpha * crossing + alpha * alpha * squared
    new_image = image + alpha * direction
    new_direction = new_residual + norm_next / norm_now * direction
    return (new_image, new_residual, new_direction)


def solution(mesh):
    rows = P("spoke", None, None, None)
    in_specs = (rows, rows, rows, P(None, "coil", None, None, None), P("spoke", None, None), P("spoke"))
    return jax.shard_map(shards, mesh=mesh, in_specs=in_specs, out_specs=(rows, rows, rows), check_vma=False)
```

```python
import math

import jax
import jax.numpy as jnp
import numpy as np
from jax import lax
from jax.experimental import pallas as pl
from jax.experimental.pallas import tpu as pltpu
from jax.sharding import PartitionSpec as P

F32, BF16 = jnp.float32, jnp.bfloat16
MESH = pl.DeviceIdType.MESH
ridge = 0.1


class Place:
    def __init__(self):
        self.coil = lax.axis_index("coil")
        self.spoke = lax.axis_index("spoke")
        self.core = self.spoke % 2
        self.x = (self.spoke // 2) % 4
        self.hi = (self.spoke // 8) % 2
        self.y = self.spoke // 16
        self.z = self.hi * 4 + self.coil
        self.sibling = self.spoke + 1 - 2 * self.core
        self.other = self.spoke + 8 - 16 * self.hi

    def chip(self, j):
        q = (self.y * 4 + self.x + j) % 16
        return (q // 4) * 16 + self.hi * 8 + (q % 4) * 2 + self.core

    def in_plane(self, j):
        return (self.y * 8 + self.x * 2 + self.core + j) % 32


def spoke_of(q, hi):
    return (q // 8) * 16 + hi * 8 + q % 8


def signal(device):
    pl.semaphore_signal(pltpu.get_barrier_semaphore(), inc=1, device_id=device, device_id_type=MESH)


def remote(src, dst, send_sem, recv_sem, device):
    return pltpu.make_async_remote_copy(
        src_ref=src, dst_ref=dst, send_sem=send_sem, recv_sem=recv_sem,
        device_id=device, device_id_type=MESH,
    )


def wave_block():
    n = 256
    q = (np.arange(n)[:, None] * np.arange(n)[None, :]) % n
    ang = q.astype(np.float32) * np.float32(2.0 * math.pi / n)
    c = (np.cos(ang) * np.float32(1.0 / math.sqrt(n))).astype(jnp.bfloat16)
    s = (np.sin(ang) * np.float32(1.0 / math.sqrt(n))).astype(jnp.bfloat16)
    return np.concatenate([np.concatenate([c, s], 1), np.concatenate([-s, c], 1)], 0)

def dot(a, b, dims=(((1,), (0,)), ((), ()))):
    return lax.dot_general(a, b, dims, preferred_element_type=F32)

def tables(tile_ref, wave, tf, tft):
    row = lax.broadcasted_iota(jnp.int32, (8, 256), 0)
    column = lax.broadcasted_iota(jnp.int32, (8, 256), 1)
    picks = [jnp.where(column == tile_ref[b] * 8 + row, 1.0, 0.0) for b in range(8)]
    pick = jnp.concatenate(picks, 0).astype(BF16)
    tf[:64, :] = dot(pick, wave[:256, :]).astype(BF16)
    tf[64:, :] = dot(pick, wave[256:, :]).astype(BF16)
    tft[...] = tf[...].astype(F32).T.astype(BF16)


def unpack_direction(dirg, d):
    for h in range(2):
        for q in range(4):
            for r in range(4):
                d[q, h, pl.ds(r, 64, stride=4), :] = dirg[h, pl.ds(r * 4 + q, 64, stride=16), :]

def map_rows(mv, g, k):
    v = mv[g, k].astype(F32)
    return v[0:1].reshape(8, 128), v[1:2].reshape(8, 128)

def forward_pass(mv, d, tf, tr, ti):
    def forward(i, carry):
        p, c = i // 8, i % 8
        re, im = [], []
        for h in range(2):
            cr, ci = [], []
            for g in range(32):
                mr, mi = map_rows(mv, g, c * 4 + p * 2 + h)
                dr = d[2 * p, h, g * 8:(g + 1) * 8, :]
                di = d[2 * p + 1, h, g * 8:(g + 1) * 8, :]
                cr.append(mr * dr - mi * di)
                ci.append(mr * di + mi * dr)
            re.append(jnp.concatenate(cr, 0).astype(BF16))
            im.append(jnp.concatenate(ci, 0).astype(BF16))
        t = dot(tf[:, :256], jnp.concatenate(re, 1)) + dot(tf[:, 256:], jnp.concatenate(im, 1))
        rows = pl.ds(pl.multiple_of(i * 64, 64), 64)
        tr[rows, :] = t[:64].astype(BF16)
        ti[rows, :] = t[64:].astype(BF16)
        return carry
    lax.fori_loop(0, 16, forward, 0, unroll=4)

def halves(ks, rows, re, im):
    for h in range(2):
        ks[0, h, rows, :] = re[:, h * 128:(h + 1) * 128]
        ks[1, h, rows, :] = im[:, h * 128:(h + 1) * 128]

def strided(ks, part, rows):
    return jnp.concatenate([ks[part, 0, rows, :], ks[part, 1, rows, :]], 1)

def row_pass(wave, a_ref, b_ref, ks, inverse):
    cosm, sinm, nsinm = wave[:256, :256], wave[:256, 256:], wave[256:, :256]
    s1, s2 = (nsinm, sinm) if inverse else (sinm, nsinm)
    def row(i, carry):
        rows = pl.ds(pl.multiple_of(i * 256, 256), 256)
        a, b = a_ref[rows, :], b_ref[rows, :]
        halves(ks, rows, dot(a, cosm) + dot(b, s1), dot(a, s2) + dot(b, cosm))
        return carry
    lax.fori_loop(0, 4, row, 0)

def sample_pass(ks, wv, gr, gi):
    def block(b, carry):
        parts = []
        for r in range(8):
            rows = pl.ds(b * 8 + r, 16, stride=64)
            parts.append(jnp.concatenate([strided(ks, 0, rows), strided(ks, 1, rows)], 0).astype(BF16))
        picked = jnp.concatenate(parts, 1)
        w = wv[b]
        s = dot(picked, w, (((1,), (1,)), ((), ()))).astype(BF16)
        g = dot(s, w).astype(BF16)
        for r in range(8):
            rows = pl.ds(pl.multiple_of((b * 8 + r) * 16, 16), 16)
            gr[rows, :] = g[:16, r * 256:(r + 1) * 256]
            gi[rows, :] = g[16:, r * 256:(r + 1) * 256]
        return carry
    lax.fori_loop(0, 8, block, 0, unroll=2)

def combine_pass(ks, tft, mv, acc, p):
    def combine(c, carry):
        i = p * 8 + c
        rows = pl.ds(i, 64, stride=16)
        sp = jnp.concatenate([strided(ks, 0, rows), strided(ks, 1, rows)], 0).astype(BF16)
        img = dot(tft[...], sp)
        for h in range(2):
            for g in range(32):
                mr, mi = map_rows(mv, g, c * 4 + p * 2 + h)
                ir = img[g * 8:(g + 1) * 8, h * 128:(h + 1) * 128]
                ii = img[256 + g * 8:256 + (g + 1) * 8, h * 128:(h + 1) * 128]
                acc[2 * p, h, g * 8:(g + 1) * 8, :] += mr * ir + mi * ii
                acc[2 * p + 1, h, g * 8:(g + 1) * 8, :] += mr * ii - mi * ir
        return carry
    lax.fori_loop(0, 8, combine, 0, unroll=4)


def solve_kernel(tile_ref, d_ref, r_ref, m_hbm, wave_hbm, w_hbm, applied_ref, coef_ref,
                 own, dirg, dirf, d, tf, tft, tr, ti, ks, gr, gi, acc, wv, mv, wave,
                 part, came, zsend, zcame, d8, r8, row, rows,
                 load_sem, gsend, grecv, psend, precv, zsend_sem, zrecv_sem, ssend, srecv):
    here = Place()
    coil, spoke, hi, z, sibling, other = here.coil, here.spoke, here.hi, here.z, here.sibling, here.other
    me = here.in_plane(0)

    def line(j):
        to = (z + j) % 8
        return to, (to % 4, spoke + 8 * (to // 4 - hi))

    def greet(j, carry):
        signal((coil, here.chip(j)))
        return carry

    def greet_line(j, carry):
        signal(line(j)[1])
        return carry

    lax.fori_loop(1, 16, greet, 0)
    lax.fori_loop(1, 8, greet_line, 0)
    signal((coil, sibling))
    loads = [pltpu.make_async_copy(wave_hbm, wave, load_sem.at[9])]
    loads += [
        pltpu.make_async_copy(m_hbm.at[:, y], mv.at[:, :, :, y * 128:(y + 1) * 128], load_sem.at[y])
        for y in range(8)
    ]
    loads.append(pltpu.make_async_copy(w_hbm, wv, load_sem.at[8]))
    for load in loads:
        load.start()
    for k in range(8):
        own[2 * k:2 * k + 2, :] = d_ref[k // 2, k % 2]
        d8[k % 2, 2 * (k // 2):2 * (k // 2) + 2, :] = d_ref[k // 2, k % 2]
        r8[k % 2, 2 * (k // 2):2 * (k // 2) + 2, :] = r_ref[k // 2, k % 2]
    dirg[spoke] = own[...]
    acc[...] = jnp.zeros_like(acc)
    pl.semaphore_wait(pltpu.get_barrier_semaphore(), 23)

    def send(src, slot, phase, j, device):
        return remote(src, dirg.at[slot], gsend.at[phase, j], grecv.at[slot], device)

    def arrived(slot):
        remote(own, dirg.at[slot], gsend.at[0, 0], grecv.at[slot], (coil, sibling)).wait_recv()

    send(own, spoke, 2, 0, (3 - coil, other)).start()

    def first(j, carry):
        send(own, spoke, 0, j, (coil, here.chip(j))).start()
        return carry

    lax.fori_loop(1, 16, first, 0)
    send(own, spoke, 0, 0, (coil, sibling)).start()
    loads[0].wait()
    tables(tile_ref, wave, tf, tft)
    arrived(other)

    def second(j, carry):
        send(dirg.at[other], other, 1, j, (coil, here.chip(j))).start()
        return carry

    lax.fori_loop(1, 16, second, 0)
    send(dirg.at[other], other, 1, 0, (coil, sibling)).start()
    flip = 8 - 16 * hi
    for phase, shift in ((2, 0), (3, flip)):
        def relay(j, carry, phase=phase, shift=shift):
            slot = here.chip(j) + shift
            arrived(slot)
            send(dirg.at[slot], slot, phase, j, (coil, sibling)).start()
            return carry

        lax.fori_loop(1, 16, relay, 0)

    def rest(j, carry):
        slot = here.chip(j) + 1 - 2 * here.core
        arrived(slot)
        arrived(slot + flip)
        return carry

    lax.fori_loop(0, 16, rest, 0)
    for h in range(2):
        dirf[h] = dirg[:, :, h * 128:(h + 1) * 128].reshape(1024, 128)
    unpack_direction(dirf, d)
    for load in loads[1:]:
        load.wait()
    forward_pass(mv, d, tf, tr, ti)
    row_pass(wave, tr, ti, ks, False)
    sample_pass(ks, wv, gr, gi)
    row_pass(wave, gr, gi, ks, True)

    def exchange(p, j):
        q = here.in_plane(j)
        return remote(part.at[p, q // 8, :, q % 8], came.at[p, me], psend.at[p, j], precv.at[p, me],
                      (coil, spoke_of(q, hi)))

    for p in range(2):
        combine_pass(ks, tft, mv, acc, p)
        for h in range(2):
            for k in range(2):
                for r in range(4):
                    dirf[h, pl.ds(r * 2 + k, 64, stride=8), :] = acc[2 * p + k, h, pl.ds(r, 64, stride=4), :]
            part[p, :, :, :, :, h * 128:(h + 1) * 128] = dirf[h, :512].astype(BF16).reshape(4, 2, 8, 8, 128)

        def start(j, carry, p=p):
            exchange(p, j).start()
            return carry

        lax.fori_loop(1, 32, start, 0)
        came[p, me] = part[p, here.y, :, here.x * 2 + here.core]

    def zcopy(p, j):
        to, device = line(j)
        return remote(zsend.at[p, to // 4], zcame.at[p, z], zsend_sem.at[p, j], zrecv_sem.at[p, z], device)

    for p in range(2):
        def came_in(j, carry, p=p):
            q = here.in_plane(j)
            remote(came.at[p, q], came.at[p, q], psend.at[p, j], precv.at[p, q], (coil, sibling)).wait_recv()
            return carry

        lax.fori_loop(1, 32, came_in, 0)
        total = came[p, 0].astype(F32)
        for q in range(1, 32):
            total = total + came[p, q].astype(F32)
        zsend[p] = total.astype(BF16)

        def zstart(j, carry, p=p):
            zcopy(p, j).start()
            return carry

        lax.fori_loop(1, 8, zstart, 0)
        zcame[p, z] = zsend[p, hi]

    applied = []
    sums = [0.0, 0.0, 0.0, 0.0]
    for p in range(2):
        def zwait(j, carry, p=p):
            frm = (z + j) % 8
            remote(zsend.at[p, 0], zcame.at[p, frm], zsend_sem.at[p, j], zrecv_sem.at[p, frm],
                   (coil, sibling)).wait_recv()
            return carry

        lax.fori_loop(1, 8, zwait, 0)
        value = zcame[p, 0].astype(F32)
        for k in range(1, 8):
            value = value + zcame[p, k].astype(F32)
        dp, rp = d8[p], r8[p]
        value = value + ridge * dp
        applied.append(value)
        for k, term in enumerate((rp * rp, dp * value, rp * value, value * value)):
            sums[k] = sums[k] + jnp.sum(term)
    lane = lax.broadcasted_iota(jnp.int32, (1, 128), 1)
    mine = jnp.zeros((1, 128), F32)
    for k in range(4):
        mine = jnp.where(lane == k, sums[k], mine)
    row[...] = mine
    rows[spoke] = mine

    def share(j):
        return remote(row, rows.at[spoke], ssend.at[j], srecv.at[spoke],
                      (coil, spoke_of(here.in_plane(j), hi)))

    def share_across(j):
        return remote(row, rows.at[spoke], ssend.at[32 + j], srecv.at[spoke],
                      (3 - coil, spoke_of(here.in_plane(j), 1 - hi)))

    def share_start(j, carry):
        share(j).start()
        return carry

    def across_start(j, carry):
        share_across(j).start()
        return carry

    lax.fori_loop(0, 32, across_start, 0)
    lax.fori_loop(1, 32, share_start, 0)
    for k in range(8):
        applied_ref[k // 2, k % 2] = applied[k % 2][2 * (k // 2):2 * (k // 2) + 2]

    def share_wait(j, carry):
        frm = (spoke + j) % 64
        remote(row, rows.at[frm], ssend.at[j], srecv.at[frm], (coil, sibling)).wait_recv()
        return carry

    lax.fori_loop(1, 64, share_wait, 0)
    total = jnp.sum(rows[...], axis=0)
    norm_now, curvature, crossing, squared = (
        jnp.sum(jnp.where(lane == k, total, 0.0), axis=1, keepdims=True) for k in range(4)
    )
    alpha = norm_now / curvature
    norm_next = norm_now - 2.0 * alpha * crossing + alpha * alpha * squared
    coef_ref[0:1, :] = jnp.broadcast_to(alpha, (1, 256))
    coef_ref[1:2, :] = jnp.broadcast_to(norm_next / norm_now, (1, 256))
    for phase in range(4):
        def gsent(j, carry, phase=phase):
            send(own, spoke, phase, j, (coil, sibling)).wait_send()
            return carry

        lax.fori_loop(1 if phase == 3 else 0, 16, gsent, 0)

    def sent(j, carry):
        exchange(0, j).wait_send()
        exchange(1, j).wait_send()
        share(j).wait_send()
        return carry

    def zsent(j, carry):
        zcopy(0, j).wait_send()
        zcopy(1, j).wait_send()
        return carry

    def across_sent(j, carry):
        share_across(j).wait_send()
        return carry

    lax.fori_loop(1, 32, sent, 0)
    lax.fori_loop(1, 8, zsent, 0)
    lax.fori_loop(0, 32, across_sent, 0)


def solve_call(tile_index, direction, residual, maps, wave, w):
    vm = pl.BlockSpec(memory_space=pltpu.VMEM)
    hbm = pl.BlockSpec(memory_space=pl.ANY)
    dma = pltpu.SemaphoreType.DMA
    return pl.pallas_call(
        solve_kernel,
        out_shape=(jax.ShapeDtypeStruct((4, 2, 2, 256), F32), jax.ShapeDtypeStruct((2, 256), F32)),
        in_specs=[pl.BlockSpec(memory_space=pltpu.SMEM), vm, vm, hbm, hbm, hbm],
        out_specs=(vm, vm),
        scratch_shapes=[
            pltpu.VMEM((16, 256), F32),
            pltpu.VMEM((64, 16, 256), F32),
            pltpu.VMEM((2, 1024, 128), F32),
            pltpu.VMEM((4, 2, 256, 128), F32),
            pltpu.VMEM((128, 512), BF16),
            pltpu.VMEM((512, 128), BF16),
            pltpu.VMEM((1024, 256), BF16),
            pltpu.VMEM((1024, 256), BF16),
            pltpu.VMEM((2, 2, 1024, 128), F32),
            pltpu.VMEM((1024, 256), BF16),
            pltpu.VMEM((1024, 256), BF16),
            pltpu.VMEM((4, 2, 256, 128), F32),
            pltpu.VMEM((8, 128, 2048), BF16),
            pltpu.VMEM((32, 32, 2, 1024), BF16),
            pltpu.VMEM((512, 512), BF16),
            pltpu.VMEM((2, 4, 2, 8, 8, 256), BF16),
            pltpu.VMEM((2, 32, 2, 8, 256), BF16),
            pltpu.VMEM((2, 2, 8, 256), BF16),
            pltpu.VMEM((2, 8, 8, 256), BF16),
            pltpu.VMEM((2, 8, 256), F32),
            pltpu.VMEM((2, 8, 256), F32),
            pltpu.VMEM((1, 128), F32),
            pltpu.VMEM((64, 1, 128), F32),
            dma((10,)), dma((4, 16)), dma((64,)), dma((2, 32)), dma((2, 32)),
            dma((2, 8)), dma((2, 8)), dma((64,)), dma((64,)),
        ],
        compiler_params=pltpu.CompilerParams(
            collective_id=0, has_side_effects=True, vmem_limit_bytes=60 * 2**20
        ),
        name="solve",
    )(tile_index, direction, residual, maps, wave, w)


def maps_view(maps):
    parts = maps.reshape(32, 8, 16, 2, 2, 128).transpose(0, 1, 2, 4, 3, 5)
    return parts.reshape(32, 8, 32, 2, 128)


def shards(image, residual, direction, coil_maps, interp_weights, tile_index):
    applied, coef = solve_call(
        tile_index, direction, residual, maps_view(coil_maps), jnp.asarray(wave_block()), interp_weights
    )
    new_residual = residual - coef[0] * applied
    new_image = image + coef[0] * direction
    new_direction = new_residual + coef[1] * direction
    return (new_image, new_residual, new_direction)


def solution(mesh):
    rows = P("spoke", None, None, None)
    in_specs = (rows, rows, rows, P(None, "coil", None, None, None), P("spoke", None, None), P("spoke"))
    return jax.shard_map(shards, mesh=mesh, in_specs=in_specs, out_specs=(rows, rows, rows), check_vma=False)
```

```python
import math

import jax
import jax.numpy as jnp
import numpy as np
from jax import lax
from jax.experimental import pallas as pl
from jax.experimental.pallas import tpu as pltpu
from jax.sharding import PartitionSpec as P

F32, BF16 = jnp.float32, jnp.bfloat16
MESH = pl.DeviceIdType.MESH
NT = (((1,), (1,)), ((), ()))
ridge = 0.1
RING = (2, 1, 3, 0)
STEPS = sorted(((j, i) for j in range(4) for i in range(4)), key=lambda s: -min(s[0], 4 - s[0]) - min(s[1], 4 - s[1]))


class Place:
    def __init__(self):
        self.coil = lax.axis_index("coil")
        self.spoke = lax.axis_index("spoke")
        self.core = self.spoke % 2
        x = (self.spoke // 2) % 4
        self.hi = (self.spoke // 8) % 2
        y = self.spoke // 16
        self.z = self.hi * 4 + self.coil
        self.sibling = self.spoke + 1 - 2 * self.core
        self.flip = 8 - 16 * self.hi
        self.ys = [(y + j) % 4 for j in range(4)]
        self.xs = [((x + j) % 4) * 2 for j in range(4)]
        self.cores = [self.core, 1 - self.core]
        self.rows = [v * 16 + self.hi * 8 for v in self.ys]

    def chip(self, step):
        return self.rows[step[0]] + self.xs[step[1]] + self.core

    def line(self, j):
        to = (self.z + j) % 8
        return to // 4, (to % 4, self.spoke + 8 * (to // 4 - self.hi))


def signal(device):
    pl.semaphore_signal(pltpu.get_barrier_semaphore(), inc=1, device_id=device, device_id_type=MESH)


def remote(src, dst, send_sem, recv_sem, device):
    return pltpu.make_async_remote_copy(
        src_ref=src, dst_ref=dst, send_sem=send_sem, recv_sem=recv_sem,
        device_id=device, device_id_type=MESH,
    )


def wave_block():
    n = 256
    q = (np.arange(n)[:, None] * np.arange(n)[None, :]) % n
    ang = q.astype(np.float32) * np.float32(2.0 * math.pi / n)
    c = (np.cos(ang) * np.float32(1.0 / math.sqrt(n))).astype(jnp.bfloat16)
    s = (np.sin(ang) * np.float32(1.0 / math.sqrt(n))).astype(jnp.bfloat16)
    return np.concatenate([np.concatenate([c, s], 1), np.concatenate([-s, c], 1)], 0)


def wave_columns():
    return np.arange(512).reshape(2, 4, 2, 32).transpose(2, 0, 1, 3).reshape(-1)


def dot(a, b, dims=(((1,), (0,)), ((), ()))):
    return lax.dot_general(a, b, dims, preferred_element_type=F32)


def tables(tile_ref, wave, tf, tft):
    row = lax.broadcasted_iota(jnp.int32, (8, 256), 0)
    column = lax.broadcasted_iota(jnp.int32, (8, 256), 1)
    picks = [jnp.where(column == tile_ref[b] * 8 + row, 1.0, 0.0) for b in range(8)]
    pick = jnp.concatenate(picks, 0).astype(BF16)
    tf[:64, :] = dot(pick, wave[:256, :]).astype(BF16)
    tf[64:, :] = dot(pick, wave[256:, :]).astype(BF16)
    tft[...] = tf[...].astype(F32).T.astype(BF16)


def unpack_direction(dirg, d, side):
    for y in range(4):
        base = pl.multiple_of((y * 2 + side) * 256, 256)
        for h in range(2):
            for q in range(4):
                for r in range(4):
                    d[q, h, pl.ds(y * 32 + r, 8, stride=4), :] = dirg[pl.ds(base + h * 16 + r * 4 + q, 8, stride=32), :]


def map_rows(mv, g, k):
    v = mv[g, k].astype(F32)
    return v[0:1].reshape(8, 128), v[1:2].reshape(8, 128)


def forward_terms(mv, d, tf, side, i):
    p, c = i // 8, i % 8
    re, im = [], []
    for h in range(2):
        cr, ci = [], []
        for g in range(16):
            mr, mi = map_rows(mv, (g // 4) * 8 + side * 4 + g % 4, c * 4 + p * 2 + h)
            dr = d[2 * p, h, g * 8:(g + 1) * 8, :]
            di = d[2 * p + 1, h, g * 8:(g + 1) * 8, :]
            cr.append(mr * dr - mi * di)
            ci.append(mr * di + mi * dr)
        re.append(jnp.concatenate(cr, 0).astype(BF16))
        im.append(jnp.concatenate(ci, 0).astype(BF16))
    coil = jnp.concatenate([jnp.concatenate(re, 1), jnp.concatenate(im, 1)], 0)
    return dot(tf[:, pl.ds(pl.multiple_of(side * 256, 256), 256)], coil)


def halves(ks, rows, re, im):
    for h in range(2):
        ks[0, h, rows, :] = re[:, h * 128:(h + 1) * 128]
        ks[1, h, rows, :] = im[:, h * 128:(h + 1) * 128]


def strided(ks, part, rows):
    return jnp.concatenate([ks[part, 0, rows, :], ks[part, 1, rows, :]], 1)


def row_pass(wave, a_ref, b_ref, ks, inverse):
    cosm, sinm, nsinm = wave[:256, :256], wave[:256, 256:], wave[256:, :256]
    s1, s2 = (nsinm, sinm) if inverse else (sinm, nsinm)
    for i in range(4):
        rows = pl.ds(i * 256, 256)
        a, b = a_ref[rows, :], b_ref[rows, :]
        halves(ks, rows, dot(a, cosm) + dot(b, s1), dot(a, s2) + dot(b, cosm))


def sample_pass(ks, wv, gr, gi):
    samples = []
    for b in range(8):
        parts = []
        for r in range(8):
            rows = pl.ds(b * 8 + r, 16, stride=64)
            parts.append(jnp.concatenate([strided(ks, 0, rows), strided(ks, 1, rows)], 0).astype(BF16))
        samples.append(dot(jnp.concatenate(parts, 1), wv[b], NT).astype(BF16))
    for b in range(8):
        g = dot(samples[b], wv[b]).astype(BF16)
        for r in range(8):
            rows = pl.ds((b * 8 + r) * 16, 16)
            gr[rows, :] = g[:16, r * 256:(r + 1) * 256]
            gi[rows, :] = g[16:, r * 256:(r + 1) * 256]


def spread_pass(ks, sp):
    for i in range(16):
        rows = pl.ds(i, 64, stride=16)
        sp[i] = jnp.concatenate([strided(ks, 0, rows), strided(ks, 1, rows)], 0).astype(BF16)


def combine_rows(sp, tft, mv, acc, stage, part, y):
    table = jnp.concatenate(
        [tft[pl.ds(pl.multiple_of(s * 256 + k * 128 + y * 32, 32), 32), :] for k in range(2) for s in range(2)], 0
    )

    def plane(p, carry):
        re = [[None] * 8, [None] * 8]
        im = [[None] * 8, [None] * 8]
        for c in range(8):
            img = dot(table, sp[p * 8 + c])
            for h in range(2):
                for g in range(8):
                    mr, mi = map_rows(mv, y * 8 + g, c * 4 + p * 2 + h)
                    ir = img[g * 8:(g + 1) * 8, h * 128:(h + 1) * 128]
                    ii = img[64 + g * 8:64 + (g + 1) * 8, h * 128:(h + 1) * 128]
                    a, b = mr * ir + mi * ii, mr * ii - mi * ir
                    re[h][g] = a if c == 0 else re[h][g] + a
                    im[h][g] = b if c == 0 else im[h][g] + b
        for h in range(2):
            acc[0, h] = jnp.concatenate(re[h], 0)
            acc[1, h] = jnp.concatenate(im[h], 0)
            for s in range(2):
                for k in range(2):
                    for r in range(4):
                        stage[h, pl.ds(s * 8 + k * 4 + r, 8, stride=16), :] = acc[k, h, pl.ds(s * 32 + r, 8, stride=4), :]
            part[y, :, p, :, :, h * 128:(h + 1) * 128] = stage[h].astype(BF16).reshape(8, 2, 8, 128)
        return carry

    lax.fori_loop(0, 2, plane, 0)


def solve_kernel(tile_ref, d_hbm, r_hbm, m_hbm, wave_hbm, wavep_hbm, w_hbm, applied_ref, alpha_ref, beta_ref,
                 dv, rv, own, dirg, d, tf, tft, tacc, tr, ti, ks, gr, gi, sp, acc, stage, wv, mv, wave, wavep,
                 part, came, zsend, zcame, d8, r8, row, rows,
                 load_sem, gsend, grecv, brecv, psend, precv, zsend_sem, zrecv_sem, ssend, srecv):
    here = Place()
    coil, spoke, hi, z, sibling = here.coil, here.spoke, here.hi, here.z, here.sibling
    other = spoke + here.flip
    near = [pltpu.make_async_copy(d_hbm, dv, load_sem.at[9]), pltpu.make_async_copy(r_hbm, rv, load_sem.at[10])]
    for load in near:
        load.start()
    for step in STEPS[:15]:
        signal((coil, here.chip(step)))
    for j in (4, 3, 5, 2, 6, 1, 7):
        signal(here.line(j)[1])
    signal((coil, sibling))
    loads = [pltpu.make_async_copy(wavep_hbm, wavep, load_sem.at[11]), pltpu.make_async_copy(wave_hbm, wave, load_sem.at[12])]
    loads += [
        pltpu.make_async_copy(m_hbm.at[:, y], mv.at[:, :, :, y * 128:(y + 1) * 128], load_sem.at[y])
        for y in range(8)
    ]
    loads.append(pltpu.make_async_copy(w_hbm, wv, load_sem.at[8]))
    for load in near:
        load.wait()
    for load in loads:
        load.start()
    for r in range(4):
        for p in range(2):
            for h in range(2):
                own[h * 16 + r * 4 + p * 2:h * 16 + r * 4 + p * 2 + 2, :] = dv[r, p, :, h * 128:(h + 1) * 128]
            for k in range(2):
                d8[p, k * 4 + r:k * 4 + r + 1, :] = dv[r, p, k:k + 1, :]
                r8[p, k * 4 + r:k * 4 + r + 1, :] = rv[r, p, k:k + 1, :]

    def slot(s):
        return dirg.at[pl.ds(pl.multiple_of(s * 32, 32), 32)]

    dirg[pl.ds(pl.multiple_of(spoke * 32, 32), 32), :] = own[...]
    pl.semaphore_wait(pltpu.get_barrier_semaphore(), 23)

    def send(src, s, device, recv_sem):
        remote(src, slot(s), gsend, recv_sem, device).start()

    def arrived(s):
        remote(own, slot(s), gsend, grecv.at[s], (coil, sibling)).wait_recv()

    def relayed(k):
        sixteen = dirg.at[pl.ds(0, 512)]
        remote(sixteen, sixteen, gsend, brecv.at[k], (coil, sibling)).wait_recv()

    send(own, spoke, (3 - coil, other), grecv.at[spoke])
    for step in STEPS[:15]:
        send(own, spoke, (coil, here.chip(step)), grecv.at[spoke])
    send(own, spoke, (coil, sibling), brecv.at[0])
    loads[0].wait()
    tables(tile_ref, wavep, tf, tft)
    arrived(other)
    for step in STEPS[:15]:
        send(slot(other), other, (coil, here.chip(step)), grecv.at[other])
    send(slot(other), other, (coil, sibling), brecv.at[1])
    for step in STEPS[:15]:
        s = here.chip(step)
        arrived(s)
        send(slot(s), s, (coil, sibling), brecv.at[0])
    relayed(0)
    unpack_direction(dirg, d, hi)
    for load in loads[1:10]:
        load.wait()
    for k in range(4):
        def first_half(i, carry):
            tacc[i] = forward_terms(mv, d, tf, hi, i)
            return carry

        lax.fori_loop(4 * k, 4 * k + 4, first_half, 0, unroll=4)
        for step in STEPS[4 * k:min(4 * k + 4, 15)]:
            s = here.chip(step) + here.flip
            arrived(s)
            send(slot(s), s, (coil, sibling), brecv.at[1])
    relayed(1)
    unpack_direction(dirg, d, 1 - hi)

    def second_half(i, carry):
        t = tacc[i] + forward_terms(mv, d, tf, 1 - hi, i)
        where = pl.ds(pl.multiple_of(i * 64, 64), 64)
        tr[where, :] = t[:64].astype(BF16)
        ti[where, :] = t[64:].astype(BF16)
        return carry

    lax.fori_loop(0, 16, second_half, 0, unroll=4)
    row_pass(wave, tr, ti, ks, False)
    loads[10].wait()
    sample_pass(ks, wv, gr, gi)
    row_pass(wave, gr, gi, ks, True)
    spread_pass(ks, sp)
    me = here.ys[0] * 8 + here.xs[0] + here.core
    for j in RING:
        y = here.ys[j]
        combine_rows(sp, tft, mv, acc, stage, part, y)
        for i in RING:
            for k in (1, 0):
                if (j, i, k) == (0, 0, 0):
                    continue
                xc = here.xs[i] + here.cores[k]
                remote(part.at[y, xc], came.at[me], psend, precv, (coil, here.rows[j] + xc)).start()
    came[me] = part[here.ys[0], here.xs[0] + here.core]
    dirgs = dirg.at[pl.ds(0, 63 * 32)]
    remote(dirgs, dirgs, gsend, brecv.at[0], (coil, sibling)).wait_send()
    others = came.at[pl.ds(0, 31)]
    remote(others, others, psend, precv, (coil, sibling)).wait_recv()
    for p in range(2):
        for s in range(2):
            total = came[0, p, s].astype(F32)
            for q in range(1, 32):
                total = total + came[q, p, s].astype(F32)
            zsend[s, p] = total.astype(BF16)
    for j in (4, 3, 5, 2, 6, 1, 7):
        s, device = here.line(j)
        remote(zsend.at[s], zcame.at[z], zsend_sem, zrecv_sem, device).start()
    zcame[z] = zsend[hi]
    remote(others, others, psend, precv, (coil, sibling)).wait_send()
    seven = zcame.at[pl.ds(0, 7)]
    remote(seven, seven, zsend_sem, zrecv_sem, (coil, sibling)).wait_recv()
    applied = []
    sums = [0.0, 0.0, 0.0, 0.0]
    for p in range(2):
        value = zcame[0, p].astype(F32)
        for k in range(1, 8):
            value = value + zcame[k, p].astype(F32)
        dp, rp = d8[p], r8[p]
        value = value + ridge * dp
        applied.append(value)
        for k, term in enumerate((rp * rp, dp * value, rp * value, value * value)):
            sums[k] = sums[k] + jnp.sum(term)
    lane = lax.broadcasted_iota(jnp.int32, (1, 128), 1)
    mine = jnp.zeros((1, 128), F32)
    for k in range(4):
        mine = jnp.where(lane == k, sums[k], mine)
    row[...] = mine
    rows[spoke] = mine
    for across in (1, 0):
        for j, i in STEPS:
            for k in (1, 0):
                if (across, j, i, k) == (0, 0, 0, 0):
                    continue
                to = here.rows[j] + here.xs[i] + here.cores[k] + across * here.flip
                where = 3 - coil if across else coil
                remote(row, rows.at[spoke], ssend, srecv, (where, to)).start()
    for r in range(4):
        for p in range(2):
            for k in range(2):
                applied_ref[r, p, k:k + 1, :] = applied[p][k * 4 + r:k * 4 + r + 1, :]
    remote(seven, seven, zsend_sem, zrecv_sem, (coil, sibling)).wait_send()
    most = rows.at[pl.ds(0, 63)]
    remote(most, most, ssend, srecv, (coil, sibling)).wait_recv()
    total = jnp.sum(rows[...], axis=0)
    norm_now, curvature, crossing, squared = (
        jnp.sum(jnp.where(lane == k, total, 0.0), axis=1, keepdims=True) for k in range(4)
    )
    alpha = norm_now / curvature
    norm_next = norm_now - 2.0 * alpha * crossing + alpha * alpha * squared
    alpha, beta = (jnp.broadcast_to(v, (2, 256)) for v in (alpha, norm_next / norm_now))
    for r in range(4):
        for p in range(2):
            alpha_ref[r, p] = alpha
            beta_ref[r, p] = beta
    remote(most, most, ssend, srecv, (coil, sibling)).wait_send()


def solve_call(tile_index, direction, residual, maps, wave, wavep, w):
    vm = pl.BlockSpec(memory_space=pltpu.VMEM)
    hbm = pl.BlockSpec(memory_space=pl.ANY)
    dma = pltpu.SemaphoreType.DMA
    block = jax.ShapeDtypeStruct((4, 2, 2, 256), F32)
    return pl.pallas_call(
        solve_kernel,
        out_shape=(block, block, block),
        in_specs=[pl.BlockSpec(memory_space=pltpu.SMEM)] + [hbm] * 6,
        out_specs=(vm, vm, vm),
        scratch_shapes=[
            pltpu.VMEM((4, 2, 2, 256), F32),
            pltpu.VMEM((4, 2, 2, 256), F32),
            pltpu.VMEM((32, 128), F32),
            pltpu.VMEM((2048, 128), F32),
            pltpu.VMEM((4, 2, 128, 128), F32),
            pltpu.VMEM((128, 512), BF16),
            pltpu.VMEM((512, 128), BF16),
            pltpu.VMEM((16, 128, 256), F32),
            pltpu.VMEM((1024, 256), BF16),
            pltpu.VMEM((1024, 256), BF16),
            pltpu.VMEM((2, 2, 1024, 128), F32),
            pltpu.VMEM((1024, 256), BF16),
            pltpu.VMEM((1024, 256), BF16),
            pltpu.VMEM((16, 128, 256), BF16),
            pltpu.VMEM((2, 2, 64, 128), F32),
            pltpu.VMEM((2, 128, 128), F32),
            pltpu.VMEM((8, 128, 2048), BF16),
            pltpu.VMEM((32, 32, 2, 1024), BF16),
            pltpu.VMEM((512, 512), BF16),
            pltpu.VMEM((512, 512), BF16),
            pltpu.VMEM((4, 8, 2, 2, 8, 256), BF16),
            pltpu.VMEM((32, 2, 2, 8, 256), BF16),
            pltpu.VMEM((2, 2, 8, 256), BF16),
            pltpu.VMEM((8, 2, 8, 256), BF16),
            pltpu.VMEM((2, 8, 256), F32),
            pltpu.VMEM((2, 8, 256), F32),
            pltpu.VMEM((1, 128), F32),
            pltpu.VMEM((64, 1, 128), F32),
            dma((13,)), dma, dma((64,)), dma((2,)), dma, dma, dma, dma, dma, dma,
        ],
        compiler_params=pltpu.CompilerParams(
            collective_id=0, has_side_effects=True, vmem_limit_bytes=60 * 2**20
        ),
        name="solve",
    )(tile_index, direction, residual, maps, wave, wavep, w)


def maps_view(maps):
    parts = maps.reshape(32, 8, 16, 2, 2, 128).transpose(0, 1, 2, 4, 3, 5)
    return parts.reshape(32, 8, 32, 2, 128)


def shards(image, residual, direction, coil_maps, interp_weights, tile_index):
    wave = wave_block()
    applied, alpha, beta = solve_call(
        tile_index, direction, residual, maps_view(coil_maps), jnp.asarray(wave),
        jnp.asarray(wave[:, wave_columns()]), interp_weights
    )
    new_residual = residual - alpha * applied
    new_image = image + alpha * direction
    new_direction = new_residual + beta * direction
    return (new_image, new_residual, new_direction)


def solution(mesh):
    rows = P("spoke", None, None, None)
    in_specs = (rows, rows, rows, P(None, "coil", None, None, None), P("spoke", None, None), P("spoke"))
    return jax.shard_map(shards, mesh=mesh, in_specs=in_specs, out_specs=(rows, rows, rows), check_vma=False)
```

```python
import math

import jax
import jax.numpy as jnp
import numpy as np
from jax import lax
from jax.experimental import pallas as pl
from jax.experimental.pallas import tpu as pltpu
from jax.sharding import PartitionSpec as P

F32, BF16 = jnp.float32, jnp.bfloat16
MESH = pl.DeviceIdType.MESH
NT = (((1,), (1,)), ((), ()))
ridge = 0.1
RING = (2, 1, 3, 0)
STEPS = sorted(((j, i) for j in range(4) for i in range(4)), key=lambda s: -min(s[0], 4 - s[0]) - min(s[1], 4 - s[1]))


class Place:
    def __init__(self):
        self.coil = lax.axis_index("coil")
        self.spoke = lax.axis_index("spoke")
        self.core = self.spoke % 2
        x = (self.spoke // 2) % 4
        self.hi = (self.spoke // 8) % 2
        y = self.spoke // 16
        self.z = self.hi * 4 + self.coil
        self.sibling = self.spoke + 1 - 2 * self.core
        self.flip = 8 - 16 * self.hi
        self.ys = [(y + j) % 4 for j in range(4)]
        self.xs = [((x + j) % 4) * 2 for j in range(4)]
        self.cores = [self.core, 1 - self.core]
        self.rows = [v * 16 + self.hi * 8 for v in self.ys]

    def chip(self, step):
        return self.rows[step[0]] + self.xs[step[1]] + self.core

    def line(self, j):
        to = (self.z + j) % 8
        return to // 4, (to % 4, self.spoke + 8 * (to // 4 - self.hi))


def signal(device):
    pl.semaphore_signal(pltpu.get_barrier_semaphore(), inc=1, device_id=device, device_id_type=MESH)


def remote(src, dst, send_sem, recv_sem, device):
    return pltpu.make_async_remote_copy(
        src_ref=src, dst_ref=dst, send_sem=send_sem, recv_sem=recv_sem,
        device_id=device, device_id_type=MESH,
    )


def wave_block():
    n = 256
    q = (np.arange(n)[:, None] * np.arange(n)[None, :]) % n
    ang = q.astype(np.float32) * np.float32(2.0 * math.pi / n)
    c = (np.cos(ang) * np.float32(1.0 / math.sqrt(n))).astype(jnp.bfloat16)
    s = (np.sin(ang) * np.float32(1.0 / math.sqrt(n))).astype(jnp.bfloat16)
    return np.concatenate([np.concatenate([c, s], 1), np.concatenate([-s, c], 1)], 0)


def wave_columns():
    return np.arange(512).reshape(2, 4, 2, 32).transpose(2, 0, 1, 3).reshape(-1)


def dot(a, b, dims=(((1,), (0,)), ((), ()))):
    return lax.dot_general(a, b, dims, preferred_element_type=F32)


def tables(tile_ref, wave, tf, tft):
    row = lax.broadcasted_iota(jnp.int32, (8, 256), 0)
    column = lax.broadcasted_iota(jnp.int32, (8, 256), 1)
    picks = [jnp.where(column == tile_ref[b] * 8 + row, 1.0, 0.0) for b in range(8)]
    pick = jnp.concatenate(picks, 0).astype(BF16)
    tf[:64, :] = dot(pick, wave[:256, :]).astype(BF16)
    tf[64:, :] = dot(pick, wave[256:, :]).astype(BF16)
    tft[...] = tf[...].astype(F32).T.astype(BF16)


def unpack_direction(dirg, d, side):
    for y in range(4):
        base = (y * 2 + side) * 320
        for h in range(2):
            for q in range(4):
                for r in range(4):
                    d[q, h, pl.ds(y * 32 + r, 8, stride=4), :] = dirg[pl.ds(base + h * 16 + r * 4 + q, 8, stride=40), :]


def map_rows(mv, g, k):
    v = mv[g, k].astype(F32)
    return v[0:1].reshape(8, 128), v[1:2].reshape(8, 128)


def forward_terms(mv, d, tf, side, i):
    p, c = i // 8, i % 8
    re, im = [], []
    for h in range(2):
        cr, ci = [], []
        for g in range(16):
            mr, mi = map_rows(mv, (g // 4) * 8 + side * 4 + g % 4, c * 4 + p * 2 + h)
            dr = d[2 * p, h, g * 8:(g + 1) * 8, :]
            di = d[2 * p + 1, h, g * 8:(g + 1) * 8, :]
            cr.append(mr * dr - mi * di)
            ci.append(mr * di + mi * dr)
        re.append(jnp.concatenate(cr, 0).astype(BF16))
        im.append(jnp.concatenate(ci, 0).astype(BF16))
    coil = jnp.concatenate([jnp.concatenate(re, 1), jnp.concatenate(im, 1)], 0)
    return dot(tf[:, pl.ds(pl.multiple_of(side * 256, 256), 256)], coil)


def halves(ks, rows, re, im):
    for h in range(2):
        ks[0, h, rows, :] = re[:, h * 128:(h + 1) * 128]
        ks[1, h, rows, :] = im[:, h * 128:(h + 1) * 128]


def strided(ks, part, rows):
    return jnp.concatenate([ks[part, 0, rows, :], ks[part, 1, rows, :]], 1)


def row_pass(wave, a_ref, b_ref, ks, inverse):
    cosm, sinm, nsinm = wave[:256, :256], wave[:256, 256:], wave[256:, :256]
    s1, s2 = (nsinm, sinm) if inverse else (sinm, nsinm)
    for i in range(4):
        rows = pl.ds(i * 256, 256)
        a, b = a_ref[rows, :], b_ref[rows, :]
        re, im = dot(a, cosm) + dot(b, s1), dot(a, s2) + dot(b, cosm)
        size = 16 if inverse else 64
        for k in range(256 // size):
            cut = slice(k * size, (k + 1) * size)
            halves(ks, pl.ds((i * 256 // size + k) * (size + 8), size), re[cut], im[cut])


def sample_pass(ks, wv, gr, gi):
    samples = []
    for b in range(8):
        parts = []
        for r in range(8):
            rows = pl.ds(b * 8 + r, 16, stride=72)
            parts.append(jnp.concatenate([strided(ks, 0, rows), strided(ks, 1, rows)], 0).astype(BF16))
        samples.append(dot(jnp.concatenate(parts, 1), wv[b], NT).astype(BF16))
    for b in range(8):
        g = dot(samples[b], wv[b]).astype(BF16)
        for r in range(8):
            rows = pl.ds((b * 8 + r) * 16, 16)
            gr[rows, :] = g[:16, r * 256:(r + 1) * 256]
            gi[rows, :] = g[16:, r * 256:(r + 1) * 256]


def spread_pass(ks, sp):
    for i in range(16):
        rows = pl.ds(i, 64, stride=24)
        sp[i] = jnp.concatenate([strided(ks, 0, rows), strided(ks, 1, rows)], 0).astype(BF16)


def combine_rows(sp, tft, mv, acc, stage, part, y):
    table = jnp.concatenate(
        [tft[pl.ds(pl.multiple_of(s * 256 + k * 128 + y * 32, 32), 32), :] for k in range(2) for s in range(2)], 0
    )

    def plane(p, carry):
        re = [[None] * 8, [None] * 8]
        im = [[None] * 8, [None] * 8]
        for c in range(8):
            img = dot(table, sp[p * 8 + c])
            for h in range(2):
                for g in range(8):
                    mr, mi = map_rows(mv, y * 8 + g, c * 4 + p * 2 + h)
                    ir = img[g * 8:(g + 1) * 8, h * 128:(h + 1) * 128]
                    ii = img[64 + g * 8:64 + (g + 1) * 8, h * 128:(h + 1) * 128]
                    a, b = mr * ir + mi * ii, mr * ii - mi * ir
                    re[h][g] = a if c == 0 else re[h][g] + a
                    im[h][g] = b if c == 0 else im[h][g] + b
        for h in range(2):
            acc[0, h] = jnp.concatenate(re[h], 0)
            acc[1, h] = jnp.concatenate(im[h], 0)
            for s in range(2):
                for k in range(2):
                    for r in range(4):
                        stage[h, pl.ds(s * 8 + k * 4 + r, 8, stride=24), :] = acc[k, h, pl.ds(s * 32 + r, 8, stride=4), :]
            dense = jnp.concatenate([stage[h, i * 24:i * 24 + 16, :] for i in range(8)], 0)
            part[y, :, :, p, :, :, h * 128:(h + 1) * 128] = dense.astype(BF16).reshape(4, 2, 2, 8, 128)
        return carry

    lax.fori_loop(0, 2, plane, 0)


def solve_kernel(tile_hbm, d_hbm, r_hbm, m_hbm, wave_hbm, wavep_hbm, w_hbm, applied_ref, alpha_ref, beta_ref,
                 tile_ref, dv, rv, own, dirg, d, tf, tft, tacc, tr, ti, ks, gr, gi, sp, acc, stage, wv, mv, wave, wavep,
                 part, half, pair, came, zsend, zcame, d8, r8, row, rows,
                 load_sem, gsend, grecv, brecv, asend, hsend, hrecv, psend, precv, zsend_sem, zrecv_sem, ssend, srecv, esend):
    here = Place()
    coil, spoke, hi, z, sibling = here.coil, here.spoke, here.hi, here.z, here.sibling
    other = spoke + here.flip
    near = [pltpu.make_async_copy(d_hbm, dv, load_sem.at[9]), pltpu.make_async_copy(r_hbm, rv, load_sem.at[10])]
    near.append(pltpu.make_async_copy(tile_hbm, tile_ref, load_sem.at[13]))
    for load in near:
        load.start()
    for step in STEPS[:15]:
        signal((coil, here.chip(step)))
    for j in (4, 3, 5, 2, 6, 1, 7):
        signal(here.line(j)[1])
    signal((coil, sibling))
    loads = [pltpu.make_async_copy(wavep_hbm, wavep, load_sem.at[11]), pltpu.make_async_copy(wave_hbm, wave, load_sem.at[12])]
    loads += [
        pltpu.make_async_copy(m_hbm.at[:, y], mv.at[:, :, :, y * 128:(y + 1) * 128], load_sem.at[y])
        for y in range(8)
    ]
    loads.append(pltpu.make_async_copy(w_hbm, wv, load_sem.at[8]))
    for load in near:
        load.wait()
    for load in loads:
        load.start()
    for r in range(4):
        for p in range(2):
            for h in range(2):
                own[h * 16 + r * 4 + p * 2:h * 16 + r * 4 + p * 2 + 2, :] = dv[r, p, :, h * 128:(h + 1) * 128]
            for k in range(2):
                d8[p, k * 4 + r:k * 4 + r + 1, :] = dv[r, p, k:k + 1, :]
                r8[p, k * 4 + r:k * 4 + r + 1, :] = rv[r, p, k:k + 1, :]

    def slot(s):
        return dirg.at[pl.ds(pl.multiple_of(s * 40, 8), 32)]

    dirg[pl.ds(pl.multiple_of(spoke * 40, 8), 32), :] = own[...]
    pl.semaphore_wait(pltpu.get_barrier_semaphore(), 23)

    def send(src, s, device, recv_sem):
        remote(src, slot(s), gsend, recv_sem, device).start()

    def arrived(s):
        remote(own, slot(s), gsend, grecv.at[s], (coil, sibling)).wait_recv()

    def relayed(k):
        sixteen = dirg.at[pl.ds(0, 512)]
        remote(sixteen, sixteen, gsend, brecv.at[k], (coil, sibling)).wait_recv()

    edge = coil % 3 == 0
    nearest = (3 - coil, 2 - coil // 3)

    @pl.when(edge)
    def _():
        for to in nearest:
            remote(own, slot(spoke), asend, grecv.at[spoke], (to, other)).start()

    for step in STEPS[:15]:
        send(own, spoke, (coil, here.chip(step)), grecv.at[spoke])
    send(own, spoke, (coil, sibling), brecv.at[0])
    loads[0].wait()
    tables(tile_ref, wavep, tf, tft)
    arrived(other)
    send(slot(other), other, (coil, sibling), brecv.at[1])
    for step in STEPS[:15]:
        send(slot(other), other, (coil, here.chip(step)), grecv.at[other])
    for step in STEPS[:15]:
        s = here.chip(step)
        arrived(s)
        send(slot(s), s, (coil, sibling), brecv.at[0])
    relayed(0)
    unpack_direction(dirg, d, hi)
    for load in loads[1:10]:
        load.wait()
    for k in range(4):
        def first_half(i, carry):
            tacc[i] = forward_terms(mv, d, tf, hi, i)
            return carry

        lax.fori_loop(4 * k, 4 * k + 4, first_half, 0, unroll=4)
        for step in STEPS[4 * k:min(4 * k + 4, 15)]:
            s = here.chip(step) + here.flip
            arrived(s)
            send(slot(s), s, (coil, sibling), brecv.at[1])
    relayed(1)
    unpack_direction(dirg, d, 1 - hi)

    def second_half(i, carry):
        t = tacc[i] + forward_terms(mv, d, tf, 1 - hi, i)
        where = pl.ds(pl.multiple_of(i * 64, 64), 64)
        tr[where, :] = t[:64].astype(BF16)
        ti[where, :] = t[64:].astype(BF16)
        return carry

    lax.fori_loop(0, 16, second_half, 0, unroll=4)
    row_pass(wave, tr, ti, ks, False)
    loads[10].wait()
    sample_pass(ks, wv, gr, gi)
    row_pass(wave, gr, gi, ks, True)
    spread_pass(ks, sp)
    core, mine_x = here.core, here.xs[0] // 2

    def swap(k, y):
        return remote(part.at[y, :, 1 - core], half.at[k], hsend, hrecv.at[k], (coil, sibling))

    for k, j in enumerate(RING):
        y = here.ys[j]
        combine_rows(sp, tft, mv, acc, stage, part, y)
        if j != 0:
            swap(k, y).start()
        if k != 0:
            before = RING[k - 1]
            swap(k - 1, here.ys[before]).wait_recv()
            for i in range(4):
                both = part[here.ys[before], i, core].astype(F32) + half[k - 1, i].astype(F32)
                pair[k - 1, i] = both.astype(BF16)
            for i in RING:
                to = here.rows[before] + here.xs[i] + core
                remote(pair.at[k - 1, here.xs[i] // 2], came.at[before * 4 + i - 4], psend, precv, (coil, to)).start()
    for i in RING:
        for k in (1, 0):
            if (i, k) == (0, 0):
                continue
            to = here.xs[i] + here.cores[k]
            remote(part.at[here.ys[0], here.xs[i] // 2, here.cores[k]], came.at[12 + i * 2 + k], psend, precv,
                   (coil, here.rows[0] + to)).start()
    came[12] = part[here.ys[0], mine_x, core]
    dirgs = dirg.at[pl.ds(0, 62 * 32)]
    remote(dirgs, dirgs, gsend, brecv.at[0], (coil, sibling)).wait_send()

    @pl.when(edge)
    def _():
        two = dirg.at[pl.ds(0, 64)]
        remote(two, two, asend, brecv.at[0], (coil, sibling)).wait_send()

    others = came.at[pl.ds(0, 19)]
    remote(others, others, psend, precv, (coil, sibling)).wait_recv()
    for p in range(2):
        for s in range(2):
            total = came[0, p, s].astype(F32)
            for q in range(1, 20):
                total = total + came[q, p, s].astype(F32)
            zsend[s, p] = total.astype(BF16)
    for j in (4, 3, 5, 2, 6, 1, 7):
        s, device = here.line(j)
        remote(zsend.at[s], zcame.at[z], zsend_sem, zrecv_sem, device).start()
    zcame[z] = zsend[hi]
    remote(others, others, psend, precv, (coil, sibling)).wait_send()
    remote(half, half, hsend, hrecv.at[0], (coil, sibling)).wait_send()
    seven = zcame.at[pl.ds(0, 7)]
    remote(seven, seven, zsend_sem, zrecv_sem, (coil, sibling)).wait_recv()
    applied = []
    sums = [0.0, 0.0, 0.0, 0.0]
    for p in range(2):
        value = zcame[0, p].astype(F32)
        for k in range(1, 8):
            value = value + zcame[k, p].astype(F32)
        dp, rp = d8[p], r8[p]
        value = value + ridge * dp
        applied.append(value)
        for k, term in enumerate((rp * rp, dp * value, rp * value, value * value)):
            sums[k] = sums[k] + jnp.sum(term)
    lane = lax.broadcasted_iota(jnp.int32, (1, 128), 1)
    mine = jnp.zeros((1, 128), F32)
    for k in range(4):
        mine = jnp.where(lane == k, sums[k], mine)
    row[...] = mine
    rows[spoke] = mine

    def share(to, sem, where):
        remote(row, rows.at[spoke], sem, srecv, (where, to)).start()

    @pl.when(edge)
    def _():
        for j, i in STEPS:
            for k in (1, 0):
                for where in nearest:
                    share(here.rows[j] + here.xs[i] + here.cores[k] + here.flip, esend, where)

    for j, i in STEPS:
        for k in (1, 0):
            if (j, i, k) != (0, 0, 0):
                share(here.rows[j] + here.xs[i] + here.cores[k], ssend, coil)
    for r in range(4):
        for p in range(2):
            for k in range(2):
                applied_ref[r, p, k:k + 1, :] = applied[p][k * 4 + r:k * 4 + r + 1, :]
    remote(seven, seven, zsend_sem, zrecv_sem, (coil, sibling)).wait_send()
    most = rows.at[pl.ds(0, 63)]
    remote(most, most, ssend, srecv, (coil, sibling)).wait_recv()
    total = jnp.sum(rows[...], axis=0)
    norm_now, curvature, crossing, squared = (
        jnp.sum(jnp.where(lane == k, total, 0.0), axis=1, keepdims=True) for k in range(4)
    )
    alpha = norm_now / curvature
    norm_next = norm_now - 2.0 * alpha * crossing + alpha * alpha * squared
    alpha, beta = (jnp.broadcast_to(v, (2, 256)) for v in (alpha, norm_next / norm_now))
    for r in range(4):
        for p in range(2):
            alpha_ref[r, p] = alpha
            beta_ref[r, p] = beta
    plane = rows.at[pl.ds(0, 31)]
    remote(plane, plane, ssend, srecv, (coil, sibling)).wait_send()

    @pl.when(edge)
    def _():
        remote(rows, rows, esend, srecv, (coil, sibling)).wait_send()


def solve_call(tile_index, direction, residual, maps, wave, wavep, w):
    vm = pl.BlockSpec(memory_space=pltpu.VMEM)
    hbm = pl.BlockSpec(memory_space=pl.ANY)
    dma = pltpu.SemaphoreType.DMA
    block = jax.ShapeDtypeStruct((4, 2, 2, 256), F32)
    return pl.pallas_call(
        solve_kernel,
        out_shape=(block, block, block),
        in_specs=[hbm] * 7,
        out_specs=(vm, vm, vm),
        scratch_shapes=[
            pltpu.SMEM((8,), jnp.int32),
            pltpu.VMEM((4, 2, 2, 256), F32),
            pltpu.VMEM((4, 2, 2, 256), F32),
            pltpu.VMEM((32, 128), F32),
            pltpu.VMEM((64 * 40, 128), F32),
            pltpu.VMEM((4, 2, 128, 128), F32),
            pltpu.VMEM((128, 512), BF16),
            pltpu.VMEM((512, 128), BF16),
            pltpu.VMEM((16, 128, 256), F32),
            pltpu.VMEM((1024, 256), BF16),
            pltpu.VMEM((1024, 256), BF16),
            pltpu.VMEM((2, 2, 64 * 24, 128), F32),
            pltpu.VMEM((1024, 256), BF16),
            pltpu.VMEM((1024, 256), BF16),
            pltpu.VMEM((16, 128, 256), BF16),
            pltpu.VMEM((2, 2, 64, 128), F32),
            pltpu.VMEM((2, 192, 128), F32),
            pltpu.VMEM((8, 128, 2048), BF16),
            pltpu.VMEM((32, 32, 2, 1024), BF16),
            pltpu.VMEM((512, 512), BF16),
            pltpu.VMEM((512, 512), BF16),
            pltpu.VMEM((4, 4, 2, 2, 2, 8, 256), BF16),
            pltpu.VMEM((3, 4, 2, 2, 8, 256), BF16),
            pltpu.VMEM((3, 4, 2, 2, 8, 256), BF16),
            pltpu.VMEM((20, 2, 2, 8, 256), BF16),
            pltpu.VMEM((2, 2, 8, 256), BF16),
            pltpu.VMEM((8, 2, 8, 256), BF16),
            pltpu.VMEM((2, 8, 256), F32),
            pltpu.VMEM((2, 8, 256), F32),
            pltpu.VMEM((1, 128), F32),
            pltpu.VMEM((64, 1, 128), F32),
            dma((14,)), dma, dma((64,)), dma((2,)), dma, dma, dma((3,)), dma, dma, dma, dma, dma, dma, dma,
        ],
        compiler_params=pltpu.CompilerParams(
            collective_id=0, has_side_effects=True, vmem_limit_bytes=32 * 2**20
        ),
        name="solve",
    )(*(pltpu.with_memory_space_constraint(v, pltpu.HBM) for v in (tile_index, direction, residual, maps, wave, wavep, w)))


def maps_view(maps):
    parts = maps.reshape(32, 8, 16, 2, 2, 128).transpose(0, 1, 2, 4, 3, 5)
    return parts.reshape(32, 8, 32, 2, 128)


def shards(image, residual, direction, coil_maps, interp_weights, tile_index):
    wave = wave_block()
    applied, alpha, beta = solve_call(
        tile_index, direction, residual, maps_view(coil_maps), jnp.asarray(wave),
        jnp.asarray(wave[:, wave_columns()]), interp_weights
    )
    new_residual = residual - alpha * applied
    new_image = image + alpha * direction
    new_direction = new_residual + beta * direction
    return (new_image, new_residual, new_direction)


def solution(mesh):
    rows = P("spoke", None, None, None)
    in_specs = (rows, rows, rows, P(None, "coil", None, None, None), P("spoke", None, None), P("spoke"))
    return jax.shard_map(shards, mesh=mesh, in_specs=in_specs, out_specs=(rows, rows, rows), check_vma=False)
```

```python
import math

import jax
import jax.numpy as jnp
import numpy as np
from jax import lax
from jax.experimental import pallas as pl
from jax.experimental.pallas import tpu as pltpu
from jax.sharding import PartitionSpec as P

F32, BF16 = jnp.float32, jnp.bfloat16
MESH = pl.DeviceIdType.MESH
NT = (((1,), (1,)), ((), ()))
ridge = 0.1
RING = (2, 1, 3, 0)
STEPS = sorted(((j, i) for j in range(4) for i in range(4)), key=lambda s: -min(s[0], 4 - s[0]) - min(s[1], 4 - s[1]))


class Place:
    def __init__(self):
        self.coil = lax.axis_index("coil")
        self.spoke = lax.axis_index("spoke")
        self.core = self.spoke % 2
        x = (self.spoke // 2) % 4
        self.hi = (self.spoke // 8) % 2
        y = self.spoke // 16
        self.z = self.hi * 4 + self.coil
        self.sibling = self.spoke + 1 - 2 * self.core
        self.flip = 8 - 16 * self.hi
        self.ys = [(y + j) % 4 for j in range(4)]
        self.xs = [((x + j) % 4) * 2 for j in range(4)]
        self.cores = [self.core, 1 - self.core]
        self.rows = [v * 16 + self.hi * 8 for v in self.ys]

    def chip(self, step):
        return self.rows[step[0]] + self.xs[step[1]] + self.core

    def line(self, j):
        to = (self.z + j) % 8
        return to // 4, (to % 4, self.spoke + 8 * (to // 4 - self.hi))


def signal(device):
    pl.semaphore_signal(pltpu.get_barrier_semaphore(), inc=1, device_id=device, device_id_type=MESH)


def remote(src, dst, send_sem, recv_sem, device):
    return pltpu.make_async_remote_copy(
        src_ref=src, dst_ref=dst, send_sem=send_sem, recv_sem=recv_sem,
        device_id=device, device_id_type=MESH,
    )


def wave_block():
    n = 256
    q = (np.arange(n)[:, None] * np.arange(n)[None, :]) % n
    ang = q.astype(np.float32) * np.float32(2.0 * math.pi / n)
    c = (np.cos(ang) * np.float32(1.0 / math.sqrt(n))).astype(jnp.bfloat16)
    s = (np.sin(ang) * np.float32(1.0 / math.sqrt(n))).astype(jnp.bfloat16)
    return np.concatenate([np.concatenate([c, s], 1), np.concatenate([-s, c], 1)], 0)


def wave_columns():
    return np.arange(512).reshape(2, 4, 2, 32).transpose(2, 0, 1, 3).reshape(-1)


def dot(a, b, dims=(((1,), (0,)), ((), ()))):
    return lax.dot_general(a, b, dims, preferred_element_type=F32)


def tables(tile_ref, wave, tf, tft):
    row = lax.broadcasted_iota(jnp.int32, (8, 256), 0)
    column = lax.broadcasted_iota(jnp.int32, (8, 256), 1)
    picks = [jnp.where(column == tile_ref[b] * 8 + row, 1.0, 0.0) for b in range(8)]
    pick = jnp.concatenate(picks, 0).astype(BF16)
    tf[:64, :] = dot(pick, wave[:256, :]).astype(BF16)
    tf[64:, :] = dot(pick, wave[256:, :]).astype(BF16)
    tft[...] = tf[...].astype(F32).T.astype(BF16)


def unpack_direction(dirg, d, side):
    for y in range(4):
        base = (y * 2 + side) * 320
        for h in range(2):
            for q in range(4):
                for r in range(4):
                    d[q, h, pl.ds(y * 32 + r, 8, stride=4), :] = dirg[pl.ds(base + h * 16 + r * 4 + q, 8, stride=40), :]


def split_maps(mv, maps):
    def split(k, carry):
        for g in range(32):
            v = mv[g, k].astype(F32)
            maps[0, k, g * 8:(g + 1) * 8, :] = v[0:1].reshape(8, 128)
            maps[1, k, g * 8:(g + 1) * 8, :] = v[1:2].reshape(8, 128)
        return carry

    lax.fori_loop(0, 32, split, 0)


def map_rows(maps, k, start):
    rows = pl.ds(pl.multiple_of(start, 8), 8)
    return maps[0, k, rows, :], maps[1, k, rows, :]


def forward_terms(maps, d, tf, side, i):
    p, c = i // 8, i % 8
    re, im = [], []
    for h in range(2):
        cr, ci = [], []
        for g in range(16):
            mr, mi = map_rows(maps, c * 4 + p * 2 + h, (g // 4) * 64 + side * 32 + g % 4 * 8)
            dr = d[2 * p, h, g * 8:(g + 1) * 8, :]
            di = d[2 * p + 1, h, g * 8:(g + 1) * 8, :]
            cr.append(mr * dr - mi * di)
            ci.append(mr * di + mi * dr)
        re.append(jnp.concatenate(cr, 0).astype(BF16))
        im.append(jnp.concatenate(ci, 0).astype(BF16))
    coil = jnp.concatenate([jnp.concatenate(re, 1), jnp.concatenate(im, 1)], 0)
    return dot(tf[:, pl.ds(pl.multiple_of(side * 256, 256), 256)], coil)


def halves(ks, rows, re, im):
    for h in range(2):
        ks[0, h, rows, :] = re[:, h * 128:(h + 1) * 128]
        ks[1, h, rows, :] = im[:, h * 128:(h + 1) * 128]


def strided(ks, part, rows):
    return jnp.concatenate([ks[part, 0, rows, :], ks[part, 1, rows, :]], 1)


def row_pass(wave, a_ref, b_ref, ks, inverse):
    cosm, sinm, nsinm = wave[:256, :256], wave[:256, 256:], wave[256:, :256]
    s1, s2 = (nsinm, sinm) if inverse else (sinm, nsinm)
    for i in range(4):
        rows = pl.ds(i * 256, 256)
        a, b = a_ref[rows, :], b_ref[rows, :]
        re, im = dot(a, cosm) + dot(b, s1), dot(a, s2) + dot(b, cosm)
        size = 16 if inverse else 64
        for k in range(256 // size):
            cut = slice(k * size, (k + 1) * size)
            halves(ks, pl.ds((i * 256 // size + k) * (size + 8), size), re[cut], im[cut])


def sample_pass(ks, wv, gr, gi):
    samples = []
    for b in range(8):
        parts = []
        for r in range(8):
            rows = pl.ds(b * 8 + r, 16, stride=72)
            parts.append(jnp.concatenate([strided(ks, 0, rows), strided(ks, 1, rows)], 0).astype(BF16))
        samples.append(dot(wv[b], jnp.concatenate(parts, 1), NT).T.astype(BF16))
    for b in range(8):
        g = dot(samples[b], wv[b]).astype(BF16)
        for r in range(8):
            rows = pl.ds((b * 8 + r) * 16, 16)
            gr[rows, :] = g[:16, r * 256:(r + 1) * 256]
            gi[rows, :] = g[16:, r * 256:(r + 1) * 256]


def spread_pass(ks, sp):
    for i in range(16):
        rows = pl.ds(i, 64, stride=24)
        sp[i] = jnp.concatenate([strided(ks, 0, rows), strided(ks, 1, rows)], 0).astype(BF16)


def combine_plane(sp, tft, maps, acc, stage, part, y, p):
    table = jnp.concatenate(
        [tft[pl.ds(pl.multiple_of(s * 256 + k * 128 + y * 32, 32), 32), :] for k in range(2) for s in range(2)], 0
    )
    re = [[None] * 8, [None] * 8]
    im = [[None] * 8, [None] * 8]
    for c in range(8):
        img = dot(table, sp[p * 8 + c])
        for h in range(2):
            for g in range(8):
                mr, mi = map_rows(maps, c * 4 + p * 2 + h, y * 64 + g * 8)
                ir = img[g * 8:(g + 1) * 8, h * 128:(h + 1) * 128]
                ii = img[64 + g * 8:64 + (g + 1) * 8, h * 128:(h + 1) * 128]
                a, b = mr * ir + mi * ii, mr * ii - mi * ir
                re[h][g] = a if c == 0 else re[h][g] + a
                im[h][g] = b if c == 0 else im[h][g] + b
    for h in range(2):
        acc[p, 0, h] = jnp.concatenate(re[h], 0)
        acc[p, 1, h] = jnp.concatenate(im[h], 0)
        for s in range(2):
            for k in range(2):
                for r in range(4):
                    stage[p, h, pl.ds(s * 8 + k * 4 + r, 8, stride=24), :] = acc[p, k, h, pl.ds(s * 32 + r, 8, stride=4), :]
        dense = jnp.concatenate([stage[p, h, i * 24:i * 24 + 16, :] for i in range(8)], 0)
        part[y, :, :, p, :, :, h * 128:(h + 1) * 128] = dense.astype(BF16).reshape(4, 2, 2, 8, 128)


def solve_kernel(tile_hbm, d_hbm, r_hbm, m_hbm, wave_hbm, wavep_hbm, w_hbm, applied_ref, alpha_ref, beta_ref,
                 tile_ref, dv, rv, own, dirg, d, tf, tft, tacc, tr, ti, ks, gr, gi, sp, acc, stage, wv, mv, maps, wave, wavep,
                 part, half, pair, came, zsend, zcame, d8, r8, row, rows,
                 load_sem, gsend, grecv, brecv, asend, hsend, hrecv, psend, precv, zsend_sem, zrecv_sem, ssend, srecv, esend):
    here = Place()
    coil, spoke, hi, z, sibling = here.coil, here.spoke, here.hi, here.z, here.sibling
    other = spoke + here.flip
    near = [pltpu.make_async_copy(d_hbm, dv, load_sem.at[9]), pltpu.make_async_copy(r_hbm, rv, load_sem.at[10])]
    near.append(pltpu.make_async_copy(tile_hbm, tile_ref, load_sem.at[13]))
    for load in near:
        load.start()
    for step in STEPS[:15]:
        signal((coil, here.chip(step)))
    for j in (4, 3, 5, 2, 6, 1, 7):
        signal(here.line(j)[1])
    signal((coil, sibling))
    loads = [pltpu.make_async_copy(wavep_hbm, wavep, load_sem.at[11]), pltpu.make_async_copy(wave_hbm, wave, load_sem.at[12])]
    loads += [
        pltpu.make_async_copy(m_hbm.at[:, y], mv.at[:, :, :, y * 128:(y + 1) * 128], load_sem.at[y])
        for y in range(8)
    ]
    loads.append(pltpu.make_async_copy(w_hbm, wv, load_sem.at[8]))
    for load in near:
        load.wait()
    for load in loads:
        load.start()
    for r in range(4):
        for p in range(2):
            for h in range(2):
                own[h * 16 + r * 4 + p * 2:h * 16 + r * 4 + p * 2 + 2, :] = dv[r, p, :, h * 128:(h + 1) * 128]
            for k in range(2):
                d8[p, k * 4 + r:k * 4 + r + 1, :] = dv[r, p, k:k + 1, :]
                r8[p, k * 4 + r:k * 4 + r + 1, :] = rv[r, p, k:k + 1, :]

    def slot(s):
        return dirg.at[pl.ds(pl.multiple_of(s * 40, 8), 32)]

    dirg[pl.ds(pl.multiple_of(spoke * 40, 8), 32), :] = own[...]
    pl.semaphore_wait(pltpu.get_barrier_semaphore(), 23)

    def send(src, s, device, recv_sem):
        remote(src, slot(s), gsend, recv_sem, device).start()

    def arrived(s):
        remote(own, slot(s), gsend, grecv.at[s], (coil, sibling)).wait_recv()

    def relayed(k):
        sixteen = dirg.at[pl.ds(0, 512)]
        remote(sixteen, sixteen, gsend, brecv.at[k], (coil, sibling)).wait_recv()

    edge = coil % 3 == 0
    nearest = (3 - coil, 2 - coil // 3)

    @pl.when(edge)
    def _():
        for to in nearest:
            remote(own, slot(spoke), asend, grecv.at[spoke], (to, other)).start()

    for step in STEPS[:15]:
        send(own, spoke, (coil, here.chip(step)), grecv.at[spoke])
    send(own, spoke, (coil, sibling), brecv.at[0])
    loads[0].wait()
    tables(tile_ref, wavep, tf, tft)
    arrived(other)
    send(slot(other), other, (coil, sibling), brecv.at[1])
    for step in STEPS[:15]:
        send(slot(other), other, (coil, here.chip(step)), grecv.at[other])
    for load in loads[1:10]:
        load.wait()
    split_maps(mv, maps)
    for step in STEPS[:15]:
        s = here.chip(step)
        arrived(s)
        send(slot(s), s, (coil, sibling), brecv.at[0])
    relayed(0)
    unpack_direction(dirg, d, hi)
    for k in range(4):
        def first_half(i, carry):
            tacc[i] = forward_terms(maps, d, tf, hi, i)
            return carry

        lax.fori_loop(4 * k, 4 * k + 4, first_half, 0, unroll=4)
        for step in STEPS[4 * k:min(4 * k + 4, 15)]:
            s = here.chip(step) + here.flip
            arrived(s)
            send(slot(s), s, (coil, sibling), brecv.at[1])
    relayed(1)
    unpack_direction(dirg, d, 1 - hi)

    def second_half(i, carry):
        t = tacc[i] + forward_terms(maps, d, tf, 1 - hi, i)
        where = pl.ds(pl.multiple_of(i * 64, 64), 64)
        tr[where, :] = t[:64].astype(BF16)
        ti[where, :] = t[64:].astype(BF16)
        return carry

    lax.fori_loop(0, 16, second_half, 0, unroll=4)
    row_pass(wave, tr, ti, ks, False)
    loads[10].wait()
    sample_pass(ks, wv, gr, gi)
    row_pass(wave, gr, gi, ks, True)
    spread_pass(ks, sp)
    core, mine_x = here.core, here.xs[0] // 2

    def swap(k, y):
        return remote(part.at[y, :, 1 - core], half.at[k], hsend, hrecv.at[k], (coil, sibling))

    def send_pair(k):
        j = RING[k]
        swap(k, here.ys[j]).wait_recv()
        for i in range(4):
            pair[k, i] = (part[here.ys[j], i, core].astype(F32) + half[k, i].astype(F32)).astype(BF16)
        for i in RING:
            if (j, i) != (0, 0):
                to = here.rows[j] + here.xs[i] + core
                remote(pair.at[k, here.xs[i] // 2], came.at[k * 4 + i], psend, precv, (coil, to)).start()

    for k, j in enumerate(RING):
        y = here.ys[j]
        combine_plane(sp, tft, maps, acc, stage, part, y, 0)
        if k >= 2:
            send_pair(k - 2)
        combine_plane(sp, tft, maps, acc, stage, part, y, 1)
        swap(k, y).start()
    send_pair(2)
    send_pair(3)
    came[12] = pair[3, mine_x]
    dirgs = dirg.at[pl.ds(0, 62 * 32)]
    remote(dirgs, dirgs, gsend, brecv.at[0], (coil, sibling)).wait_send()

    @pl.when(edge)
    def _():
        two = dirg.at[pl.ds(0, 64)]
        remote(two, two, asend, brecv.at[0], (coil, sibling)).wait_send()

    others = came.at[pl.ds(0, 15)]
    remote(others, others, psend, precv, (coil, sibling)).wait_recv()
    for p in range(2):
        for s in range(2):
            total = came[0, p, s].astype(F32)
            for q in range(1, 16):
                total = total + came[q, p, s].astype(F32)
            zsend[s, p] = total.astype(BF16)
    for j in (4, 3, 5, 2, 6, 1, 7):
        s, device = here.line(j)
        remote(zsend.at[s], zcame.at[z], zsend_sem, zrecv_sem, device).start()
    zcame[z] = zsend[hi]
    remote(others, others, psend, precv, (coil, sibling)).wait_send()
    remote(half, half, hsend, hrecv.at[0], (coil, sibling)).wait_send()
    seven = zcame.at[pl.ds(0, 7)]
    remote(seven, seven, zsend_sem, zrecv_sem, (coil, sibling)).wait_recv()
    applied = []
    sums = [0.0, 0.0, 0.0, 0.0]
    for p in range(2):
        value = zcame[0, p].astype(F32)
        for k in range(1, 8):
            value = value + zcame[k, p].astype(F32)
        dp, rp = d8[p], r8[p]
        value = value + ridge * dp
        applied.append(value)
        for k, term in enumerate((rp * rp, dp * value, rp * value, value * value)):
            sums[k] = sums[k] + jnp.sum(term)
    lane = lax.broadcasted_iota(jnp.int32, (1, 128), 1)
    mine = jnp.zeros((1, 128), F32)
    for k in range(4):
        mine = jnp.where(lane == k, sums[k], mine)
    row[...] = mine
    rows[spoke] = mine

    def share(to, sem, where):
        remote(row, rows.at[spoke], sem, srecv, (where, to)).start()

    @pl.when(edge)
    def _():
        for j, i in STEPS:
            for k in (1, 0):
                for where in nearest:
                    share(here.rows[j] + here.xs[i] + here.cores[k] + here.flip, esend, where)

    for j, i in STEPS:
        for k in (1, 0):
            if (j, i, k) != (0, 0, 0):
                share(here.rows[j] + here.xs[i] + here.cores[k], ssend, coil)
    for r in range(4):
        for p in range(2):
            for k in range(2):
                applied_ref[r, p, k:k + 1, :] = applied[p][k * 4 + r:k * 4 + r + 1, :]
    remote(seven, seven, zsend_sem, zrecv_sem, (coil, sibling)).wait_send()
    most = rows.at[pl.ds(0, 63)]
    remote(most, most, ssend, srecv, (coil, sibling)).wait_recv()
    total = jnp.sum(rows[...], axis=0)
    norm_now, curvature, crossing, squared = (
        jnp.sum(jnp.where(lane == k, total, 0.0), axis=1, keepdims=True) for k in range(4)
    )
    alpha = norm_now / curvature
    norm_next = norm_now - 2.0 * alpha * crossing + alpha * alpha * squared
    alpha, beta = (jnp.broadcast_to(v, (2, 256)) for v in (alpha, norm_next / norm_now))
    for r in range(4):
        for p in range(2):
            alpha_ref[r, p] = alpha
            beta_ref[r, p] = beta
    plane = rows.at[pl.ds(0, 31)]
    remote(plane, plane, ssend, srecv, (coil, sibling)).wait_send()

    @pl.when(edge)
    def _():
        remote(rows, rows, esend, srecv, (coil, sibling)).wait_send()


def solve_call(tile_index, direction, residual, maps, wave, wavep, w):
    vm = pl.BlockSpec(memory_space=pltpu.VMEM)
    hbm = pl.BlockSpec(memory_space=pl.ANY)
    dma = pltpu.SemaphoreType.DMA
    block = jax.ShapeDtypeStruct((4, 2, 2, 256), F32)
    return pl.pallas_call(
        solve_kernel,
        out_shape=(block, block, block),
        in_specs=[hbm] * 7,
        out_specs=(vm, vm, vm),
        scratch_shapes=[
            pltpu.SMEM((8,), jnp.int32),
            pltpu.VMEM((4, 2, 2, 256), F32),
            pltpu.VMEM((4, 2, 2, 256), F32),
            pltpu.VMEM((32, 128), F32),
            pltpu.VMEM((64 * 40, 128), F32),
            pltpu.VMEM((4, 2, 128, 128), F32),
            pltpu.VMEM((128, 512), BF16),
            pltpu.VMEM((512, 128), BF16),
            pltpu.VMEM((16, 128, 256), F32),
            pltpu.VMEM((1024, 256), BF16),
            pltpu.VMEM((1024, 256), BF16),
            pltpu.VMEM((2, 2, 64 * 24, 128), F32),
            pltpu.VMEM((1024, 256), BF16),
            pltpu.VMEM((1024, 256), BF16),
            pltpu.VMEM((16, 128, 256), BF16),
            pltpu.VMEM((2, 2, 2, 64, 128), F32),
            pltpu.VMEM((2, 2, 192, 128), F32),
            pltpu.VMEM((8, 128, 2048), BF16),
            pltpu.VMEM((32, 32, 2, 1024), BF16),
            pltpu.VMEM((2, 32, 256, 128), F32),
            pltpu.VMEM((512, 512), BF16),
            pltpu.VMEM((512, 512), BF16),
            pltpu.VMEM((4, 4, 2, 2, 2, 8, 256), BF16),
            pltpu.VMEM((4, 4, 2, 2, 8, 256), BF16),
            pltpu.VMEM((4, 4, 2, 2, 8, 256), BF16),
            pltpu.VMEM((16, 2, 2, 8, 256), BF16),
            pltpu.VMEM((2, 2, 8, 256), BF16),
            pltpu.VMEM((8, 2, 8, 256), BF16),
            pltpu.VMEM((2, 8, 256), F32),
            pltpu.VMEM((2, 8, 256), F32),
            pltpu.VMEM((1, 128), F32),
            pltpu.VMEM((64, 1, 128), F32),
            dma((14,)), dma, dma((64,)), dma((2,)), dma, dma, dma((4,)), dma, dma, dma, dma, dma, dma, dma,
        ],
        compiler_params=pltpu.CompilerParams(
            collective_id=0, has_side_effects=True, vmem_limit_bytes=44 * 2**20
        ),
        name="solve",
    )(*(pltpu.with_memory_space_constraint(v, pltpu.HBM) for v in (tile_index, direction, residual, maps, wave, wavep, w)))


def maps_view(maps):
    parts = maps.reshape(32, 8, 16, 2, 2, 128).transpose(0, 1, 2, 4, 3, 5)
    return parts.reshape(32, 8, 32, 2, 128)


def shards(image, residual, direction, coil_maps, interp_weights, tile_index):
    wave = wave_block()
    applied, alpha, beta = solve_call(
        tile_index, direction, residual, maps_view(coil_maps), jnp.asarray(wave),
        jnp.asarray(wave[:, wave_columns()]), interp_weights
    )
    new_residual = residual - alpha * applied
    new_image = image + alpha * direction
    new_direction = new_residual + beta * direction
    return (new_image, new_residual, new_direction)


def solution(mesh):
    rows = P("spoke", None, None, None)
    in_specs = (rows, rows, rows, P(None, "coil", None, None, None), P("spoke", None, None), P("spoke"))
    return jax.shard_map(shards, mesh=mesh, in_specs=in_specs, out_specs=(rows, rows, rows), check_vma=False)
```
